32 devices in a mesh: mp: 4 (over z), space: 8 (over y, x, core).
Axes of the slice: x: 2, y: 2, z: 4, core: 2. Of those that a mesh axis runs over, the one named last changes fastest.
Arguments:
- positions: float32 [3, 512], P(None, 'space'), may hold values from 0 to 1
- send_lists: int32 [8, 6, 128], P('space'), may hold values from -1 to 575, as said below
- neighbours: int32 [96, 512], P(None, 'space'), may hold values from -1 to 831, as said below
- emb_scale: float32 [4, 25], P('mp'), may hold values from -4 to 4
- emb_shift: float32 [4, 25], P('mp'), may hold values from -4 to 4
- emb_middle: bfloat16 [4, 50, 25], P('mp'), may hold values from -1.25 to 1.25
- emb_mid_bias: float32 [4, 50], P('mp'), may hold values from -3 to 3
- emb_outer: bfloat16 [4, 100, 50], P('mp'), may hold values from -0.875 to 0.875
- emb_out_bias: float32 [4, 100], P('mp'), may hold values from -3 to 3
- fit_first: bfloat16 [4, 240, 1600], P('mp'), may hold values from -0.078125 to 0.078125
- fit_first_bias: float32 [4, 240], P('mp'), may hold values from -3 to 3
- fit_second: bfloat16 [4, 240, 240], P('mp'), may hold values from -0.375 to 0.375
- fit_second_bias: float32 [4, 240], P('mp'), may hold values from -3 to 3
- fit_third: bfloat16 [4, 240, 240], P('mp'), may hold values from -0.375 to 0.375
- fit_third_bias: float32 [4, 240], P('mp'), may hold values from -3 to 3
- fit_readout: bfloat16 [4, 240], P('mp'), may hold values from -0.375 to 0.375
Outputs:
- mean_force: float32 [3, 8, 4, 16], P(None, 'space', 'mp')
- force_spread: float32 [8, 4, 16], P('space', 'mp')
- virial_spread: float32 [8, 4, 16], P('space', 'mp')
The draws below stay inside these ranges and needn't reach their ends.
Inputs may be any that keep to these rules, and one draw needn't show every extreme that they name: `send_lists`: direction b runs +x, -x, +y, -y, +z, -z. A list of section b // 2 names owned atoms (below 64) or live ghost slots of earlier sections of the sender's extended array; live entries come first and -1 fills the rest; each list holds 42 to 128 live entries, entries may repeat, and in every draw some domain's list in each direction is full. `neighbours`: each entry names another owned atom of the same domain or a live ghost slot of that domain's extended array; -1 marks an empty slot.
All inputs are finite; a program needn't handle non-finite values.
Results may differ from the reference program's by a relative error of at most 0.012.
Values sent between devices are 32-bit elements; how exact they have to be, the bound alone decides.
A program may use at most 64 MiB of HBM per device.

```python
import jax
import jax.numpy as jnp
from jax import lax

E1 = 25
E2 = 50
E3 = 100
AXIS = 16
FIT = 240
K = 96
A_DEV = 64
CAP = 128
MODELS = 4
DOMAINS = 8
GY = 2
GZ = 2
ATOMS = 512
QUART = 16


def live_counts(key):
    base = jax.random.fold_in(key, 7001)
    counts = jax.random.randint(jax.random.fold_in(base, 1), (DOMAINS, 6), CAP // 3, CAP + 1)
    chosen_full = jax.random.randint(jax.random.fold_in(base, 2), (6,), 0, DOMAINS)
    row_ids = jnp.arange(DOMAINS)[:, None]
    return jnp.where(row_ids == chosen_full[None, :], CAP, counts).astype(jnp.int32)


def received_counts(counts):
    strides = (GY * GZ, GZ, 1)
    columns = []
    for block_id in range(6):
        section_id = block_id // 2
        step_by = strides[section_id] if block_id % 2 == 0 else -strides[section_id]
        columns.append(jnp.roll(counts[:, block_id], step_by, axis=0))
    return jnp.stack(columns, axis=1)


def slot_of(picked, counts, block_count):
    result = picked
    first_col = jnp.full_like(picked, A_DEV)
    for block_id in range(block_count):
        length = counts[..., block_id]
        inside = (picked >= first_col) & (picked < first_col + length)
        result = jnp.where(inside, A_DEV + block_id * CAP + (picked - first_col), result)
        first_col = first_col + length
    return result


def draw_send_lists(key, part):
    counts = live_counts(key)
    arrived = received_counts(counts)
    results = []
    for block_id in range(6):
        section_id = block_id // 2
        upper = A_DEV + jnp.sum(arrived[:, :2 * section_id], axis=1, keepdims=True)
        picked = jax.random.randint(jax.random.fold_in(key, 7100 + block_id), (DOMAINS, CAP), 0, upper)
        slots = slot_of(picked, arrived[:, None, :], 2 * section_id)
        in_use = jnp.arange(CAP)[None, :] < counts[:, block_id:block_id + 1]
        results.append(jnp.where(in_use, slots, -1))
    return jnp.stack(results, axis=1).astype(jnp.int32)


def draw_neighbours(key, part):
    counts = live_counts(key)
    arrived = received_counts(counts)
    kinds = jax.random.randint(jax.random.fold_in(key, 7201), (K, DOMAINS, A_DEV), 0, 8)
    centre = jnp.arange(A_DEV)[None, None, :]
    others = (centre + 1 + jax.random.randint(jax.random.fold_in(key, 7202), (K, DOMAINS, A_DEV), 0, A_DEV - 1)) % A_DEV
    ghost_total = jnp.sum(arrived, axis=1)
    picked = jax.random.randint(jax.random.fold_in(key, 7203), (K, DOMAINS, A_DEV), 0, ghost_total[None, :, None]) + A_DEV
    ghosts = slot_of(picked, arrived[None, :, None, :], 6)
    result = jnp.where(kinds == 0, -1, jnp.where(kinds < 4, others, ghosts))
    return result.reshape(K, ATOMS).astype(jnp.int32)


def block_scale(own_key, shape, split, least, top_value):
    def one(axis_at, parts):
        heights = jax.random.uniform(jax.random.fold_in(jax.random.fold_in(own_key, 6), axis_at), (parts,), jnp.float32, least / len(split), top_value / len(split))
        return jnp.repeat(jnp.exp(heights), shape[axis_at] // parts).reshape((-1,) + (1,) * (len(shape) - axis_at - 1))

    loudness = one(*split[0])
    for cut in split[1:]:
        loudness = loudness * one(*cut)
    return loudness


def noise(stream_key, dims, width, most, shards=(), held_as=jnp.bfloat16):
    drawn = jax.random.normal(stream_key, dims, jnp.float32) * width
    if len(shards) > 0:
        drawn = block_scale(stream_key, dims, shards, -0.22, 0.18) * drawn
    return jnp.clip(drawn, min=-most, max=most).astype(held_as)


def setup_inputs(seed: int = 0) -> dict:
    arg_keys = jax.random.split(jax.random.key(seed), 17)
    positions = jnp.clip(1.0 * jax.random.uniform(arg_keys[0], (3, ATOMS), jnp.float32) ** block_scale(arg_keys[0], (3, ATOMS), ((1, 8),), -0.2, 0.2), 0.0, 1.0)
    send_lists = draw_send_lists(jax.random.fold_in(arg_keys[16], 71), 0)
    neighbours = draw_neighbours(jax.random.fold_in(arg_keys[16], 71), 0)
    emb_scale = noise(arg_keys[3], (MODELS, E1), 1.0, 4.0, ((0, 4),), jnp.float32)
    emb_shift = noise(arg_keys[4], (MODELS, E1), 1.0, 4.0, ((0, 4),), jnp.float32)
    emb_middle = noise(arg_keys[5], (MODELS, E2, E1), E1 ** -0.5, 1.25, ((0, 4),))
    emb_mid_bias = noise(arg_keys[6], (MODELS, E2), 0.5, 3.0, ((0, 4),), jnp.float32)
    emb_outer = noise(arg_keys[7], (MODELS, E3, E2), E2 ** -0.5, 0.875, ((0, 4),))
    emb_out_bias = noise(arg_keys[8], (MODELS, E3), 0.5, 3.0, ((0, 4),), jnp.float32)
    fit_first = noise(arg_keys[9], (MODELS, FIT, E3 * AXIS), (4 * E3 * AXIS) ** -0.5, 0.078125, ((0, 4),))
    fit_first_bias = noise(arg_keys[10], (MODELS, FIT), 0.5, 3.0, ((0, 4),), jnp.float32)
    fit_second = noise(arg_keys[11], (MODELS, FIT, FIT), FIT ** -0.5, 0.375, ((0, 4),))
    fit_second_bias = noise(arg_keys[12], (MODELS, FIT), 0.5, 3.0, ((0, 4),), jnp.float32)
    fit_third = noise(arg_keys[13], (MODELS, FIT, FIT), FIT ** -0.5, 0.375, ((0, 4),))
    fit_third_bias = noise(arg_keys[14], (MODELS, FIT), 0.5, 3.0, ((0, 4),), jnp.float32)
    fit_readout = noise(arg_keys[15], (MODELS, FIT), FIT ** -0.5, 0.375, ((0, 4),))
    return dict(positions=positions, send_lists=send_lists, neighbours=neighbours, emb_scale=emb_scale, emb_shift=emb_shift, emb_middle=emb_middle, emb_mid_bias=emb_mid_bias, emb_outer=emb_outer, emb_out_bias=emb_out_bias, fit_first=fit_first, fit_first_bias=fit_first_bias, fit_second=fit_second, fit_second_bias=fit_second_bias, fit_third=fit_third, fit_third_bias=fit_third_bias, fit_readout=fit_readout)


SOFTEN = 0.04

def describe(pieces, embedding):
    offsets, present = pieces
    scale_in, shift_in, mat_two, bias_two, mat_three, bias_three = embedding
    radius_sq = lax.optimization_barrier(jnp.sum(offsets * offsets, axis=0)) + SOFTEN
    inverse = lax.rsqrt(radius_sq)
    scaled = inverse * inverse
    envelope = jnp.stack([inverse, scaled * offsets[0], scaled * offsets[1], scaled * offsets[2]]) * present[None]
    flat_inv = inverse.reshape(1, -1)
    layer_one = jnp.tanh(scale_in[:, None] * flat_inv + shift_in[:, None]).astype(jnp.bfloat16)
    pre_two = jnp.dot(mat_two, layer_one, preferred_element_type=jnp.float32) + bias_two[:, None]
    layer_two = (jnp.concatenate([layer_one, layer_one], axis=0).astype(jnp.float32) + jnp.tanh(pre_two)).astype(jnp.bfloat16)
    pre_three = jnp.dot(mat_three, layer_two, preferred_element_type=jnp.float32) + bias_three[:, None]
    layer_three = (jnp.concatenate([layer_two, layer_two], axis=0).astype(jnp.float32) + jnp.tanh(pre_three)).astype(jnp.bfloat16)
    filters = layer_three.astype(jnp.float32).reshape(layer_three.shape[0], offsets.shape[1], offsets.shape[2])
    moments = jnp.einsum('ckb,mkb->cmb', envelope, filters, precision=lax.Precision.HIGHEST) / K
    feature = jnp.einsum('cmb,cnb->mnb', moments, moments[:, :AXIS], precision=lax.Precision.HIGHEST)
    return feature.reshape(-1, offsets.shape[2]).astype(jnp.bfloat16)

def domain_energy(offsets, present, embedding, fitting):
    atom_count = offsets.shape[2]
    block_len = 128 if atom_count % 128 == 0 else atom_count
    block_total = atom_count // block_len
    shaped = offsets.reshape(3, K, block_total, block_len).transpose(2, 0, 1, 3)
    present_blocks = present.reshape(K, block_total, block_len).transpose(1, 0, 2)
    features = lax.map(lambda pieces: describe(pieces, embedding), (shaped, present_blocks))
    features = features.transpose(1, 0, 2).reshape(-1, atom_count)
    fit_one, fit_bias_one, fit_two, fit_bias_two, fit_three, fit_bias_three, readout = fitting
    hidden_one = jnp.tanh(jnp.dot(fit_one, features, preferred_element_type=jnp.float32) + fit_bias_one[:, None]).astype(jnp.bfloat16)
    hidden_two = (hidden_one.astype(jnp.float32) + jnp.tanh(jnp.dot(fit_two, hidden_one, preferred_element_type=jnp.float32) + fit_bias_two[:, None])).astype(jnp.bfloat16)
    hidden_three = (hidden_two.astype(jnp.float32) + jnp.tanh(jnp.dot(fit_three, hidden_two, preferred_element_type=jnp.float32) + fit_bias_three[:, None])).astype(jnp.bfloat16)
    return jnp.sum(jnp.dot(readout, hidden_three, preferred_element_type=jnp.float32))

def domain_terms(extended, neighbour_ids, embedding, fitting):
    owned_count = neighbour_ids.shape[1]
    ext_len = extended.shape[1]
    present = neighbour_ids >= 0
    safe_ids = jnp.where(present, neighbour_ids, ext_len)
    gathered = jnp.take(extended, safe_ids, axis=1, mode='fill', fill_value=0.0)
    offsets = gathered - extended[:, None, :owned_count]
    present_f = present.astype(jnp.float32)
    energy, pullback = jax.vjp(lambda shifted: domain_energy(shifted, present_f, embedding, fitting), offsets)
    gradient, = pullback(jnp.ones((), jnp.float32))
    virial = -(offsets[:, None] * gradient[None, :]).reshape(9, K, owned_count)
    spread_terms = jnp.concatenate([-gradient, virial], axis=0).reshape(12, -1)
    totals = jnp.zeros((12, ext_len), jnp.float32).at[:, safe_ids.reshape(-1)].add(spread_terms, mode='drop')
    centre = lax.optimization_barrier(jnp.sum(gradient, axis=1))
    return totals.at[0:3, :owned_count].add(centre)

def pick_columns(extended, chosen):
    safe_ids = jnp.where(chosen >= 0, chosen, extended.shape[1])
    return jnp.take(extended, safe_ids, axis=1, mode='fill', fill_value=0.0)

def add_columns(totals, chosen, values):
    safe_ids = jnp.where(chosen >= 0, chosen, totals.shape[1])
    return totals.at[:, safe_ids].add(values, mode='drop')

def reference(positions, send_lists, neighbours, emb_scale, emb_shift, emb_middle, emb_mid_bias, emb_outer, emb_out_bias, fit_first, fit_first_bias, fit_second, fit_second_bias, fit_third, fit_third_bias, fit_readout):
    strides = (GY * GZ, GZ, 1)
    domain_pos = positions.reshape(3, DOMAINS, A_DEV).transpose(1, 0, 2)
    domain_ids = neighbours.reshape(K, DOMAINS, A_DEV).transpose(1, 0, 2)
    extended = domain_pos
    for section_id in range(3):
        arrived = []
        for side_id in range(2):
            chosen = send_lists[:, 2 * section_id + side_id]
            payload = jax.vmap(pick_columns)(extended, chosen)
            rolled = jnp.roll(payload, strides[section_id] if side_id == 0 else -strides[section_id], axis=0)
            offset_vec = jnp.zeros((1, 3, 1), jnp.float32).at[0, section_id, 0].set(-1.0 if side_id == 0 else 1.0)
            arrived.append(rolled + offset_vec)
        extended = jnp.concatenate([extended] + arrived, axis=2)
    collected = []
    for member in range(MODELS):
        embedding = (emb_scale[member], emb_shift[member], emb_middle[member], emb_mid_bias[member], emb_outer[member], emb_out_bias[member])
        fitting = (fit_first[member], fit_first_bias[member], fit_second[member], fit_second_bias[member], fit_third[member], fit_third_bias[member], fit_readout[member])
        domain_sums = lax.map(lambda pieces: domain_terms(pieces[0], pieces[1], embedding, fitting), (extended, domain_ids))
        for section_id in (2, 1, 0):
            returned = []
            for side_id in range(2):
                first_col = A_DEV + (2 * section_id + side_id) * CAP
                ghost_block = domain_sums[:, :, first_col:first_col + CAP]
                rolled = jnp.roll(ghost_block, -strides[section_id] if side_id == 0 else strides[section_id], axis=0)
                returned.append(rolled)
            for side_id in range(2):
                domain_sums = jax.vmap(add_columns)(domain_sums, send_lists[:, 2 * section_id + side_id], returned[side_id])
        collected.append(domain_sums[:, :, :A_DEV])
    stacked = jnp.stack(collected)
    mean_all = lax.optimization_barrier(jnp.mean(stacked, axis=0))
    deviation = stacked - mean_all[None]
    force_spread = lax.optimization_barrier(jnp.mean(lax.optimization_barrier(jnp.sum(deviation[:, :, 0:3] ** 2, axis=2)), axis=0))
    virial_spread = lax.optimization_barrier(jnp.mean(lax.optimization_barrier(jnp.sum(deviation[:, :, 3:12] ** 2, axis=2)), axis=0))
    mean_force = mean_all[:, 0:3].transpose(1, 0, 2).reshape(3, DOMAINS, MODELS, QUART)
    return (mean_force, force_spread.reshape(DOMAINS, MODELS, QUART), virial_spread.reshape(DOMAINS, MODELS, QUART))
```

```python
import functools
import math

import jax
import jax.numpy as jnp
from jax import lax
from jax.experimental import pallas as pl
from jax.experimental.pallas import tpu as pltpu
from jax.sharding import PartitionSpec as P

AXIS = 16
SOFTEN = 0.04
LANES = 128
ROWS = 2
ONE = 20.0
MESH = pl.DeviceIdType.MESH
F32 = jnp.float32
BF16 = jnp.bfloat16
I32 = jnp.int32
ANY = pl.BlockSpec(memory_space=pl.ANY)
VM = pl.BlockSpec(memory_space=pltpu.VMEM)


def dims(space_count):
    grid_y = min(4, max(2, space_count // 16))
    strides = (grid_y * grid_y, grid_y, 1)
    span = (-1, 0, 1)
    found = sorted(
        {
            (a * strides[0] + b * strides[1] + c * strides[2]) % space_count
            for a in span
            for b in span
            for c in span
        }
    )
    return strides, found


def nn(a, b):
    return jnp.dot(a, b, preferred_element_type=F32)


def nt(a, b):
    return lax.dot_general(a, b, (((1,), (1,)), ((), ())), preferred_element_type=F32)


def tn(a, b):
    return lax.dot_general(a, b, (((0,), (0,)), ((), ())), preferred_element_type=F32)


def iota(shape, dim):
    return lax.broadcasted_iota(I32, shape, dim)


def hot(mask):
    return jnp.where(mask, 1.0, 0.0).astype(BF16)


def spread_of(rows, units, width, group, flip=False):
    shape = (units, rows) if flip else (rows, units)
    row = iota(shape, 1 if flip else 0)
    unit = iota(shape, 0 if flip else 1)
    inner = row % group
    return (inner < width) & (unit == (row // group) * width + inner)


def column(mask, row_value):
    return jnp.sum(jnp.where(mask, row_value, 0.0), axis=1, keepdims=True)


def rounded(value):
    return value.astype(BF16).astype(F32)


def split(value, parts):
    pieces = []
    for _ in range(parts):
        piece = value.astype(BF16)
        pieces.append(piece)
        value = value - piece.astype(F32)
    return pieces


def both(value):
    return jnp.concatenate(split(value, 2), axis=0)


def lookup(row, lane):
    return jnp.take_along_axis(
        jnp.broadcast_to(row, lane.shape), lane, axis=1, mode="promise_in_bounds"
    )


def with_bias(weight, bias, width):
    col = iota(weight.shape, 1)
    for place, piece in enumerate(split(bias, 3)):
        weight = jnp.where(col == width + place, piece.astype(F32), weight)
    return weight.astype(BF16)


def kernel(
    count, models, strides, found, sizes,
    pos_in, list_in, nb_in,
    scale_in, shift_in, mid_in, midb_in, outer_in, outb_in,
    f1_in, f1b_in, f2_in, f2b_in, f3_in, f3b_in, read_in,
    mean_ref, force_ref, virial_ref,
    pos_all, list_all, nb_ref, scale_ref, shift_ref, mid_ref, midb_ref, outer_ref, outb_ref,
    f1_ref, f1b_ref, f2_ref, f2b_ref, f3_ref, f3b_ref, read_ref,
    nscr, ptab, code_ref, f1p_ref, sel_ref, oh_ref, em_ref,
    w2_ref, w3_ref, a2_ref, a3_ref,
    off_ref, inv_ref, there_ref, id_ref, cen_ref, e4h_ref, e4l_ref,
    t1_ref, s2_ref, s3_ref, h3_ref, ms_ref, bm_ref, d_ref, dd_ref, y_ref, dms_ref,
    de4_ref, di_ref, th_ref, tl_ref, lhs_ref, part_ref, held, total, others,
    local_sem, send_a, recv_a, send_b, recv_b, send_c, recv_c, send_d, recv_d,
):
    owned, k_total, width, fit = sizes
    slots = len(found)
    group = LANES // math.gcd(k_total, LANES)
    tiles = group * k_total // LANES
    rows = owned // group
    chunks = rows // ROWS
    span = ROWS * tiles * LANES
    units = 4 * width
    g1, g2, g3 = 32, 64, 128
    pairs = ROWS * group * 4
    masks_count = (slots * owned + LANES - 1) // LANES
    me = lax.axis_index("space")
    model = lax.axis_index("mp")

    barrier = pltpu.get_barrier_semaphore()
    for off in found[1:]:
        pl.semaphore_signal(
            barrier, inc=1, device_id={"space": lax.rem(me + off, count)}, device_id_type=MESH
        )
    for step in range(1, models):
        pl.semaphore_signal(
            barrier, inc=1, device_id={"mp": lax.rem(model + step, models)}, device_id_type=MESH
        )
    moves = [
        (pos_in, pos_all.at[0]), (list_in, list_all.at[0]), (nb_in, nb_ref),
        (scale_in, scale_ref), (shift_in, shift_ref), (mid_in.at[0], mid_ref), (midb_in, midb_ref),
        (outer_in.at[0], outer_ref), (outb_in, outb_ref), (f1_in.at[0], f1_ref), (f1b_in, f1b_ref),
        (f2_in.at[0], f2_ref), (f2b_in, f2b_ref), (f3_in.at[0], f3_ref), (f3b_in, f3b_ref),
        (read_in, read_ref),
    ]
    fetched = []
    for place, (src, dst) in enumerate(moves):
        copy = pltpu.make_async_copy(src, dst, local_sem.at[place])
        copy.start()
        fetched.append(copy)
    em_ref[...] = jnp.zeros_like(em_ref)
    th_ref[...] = jnp.zeros_like(th_ref)
    tl_ref[...] = jnp.zeros_like(tl_ref)
    nscr[...] = jnp.zeros_like(nscr)
    ptab[...] = jnp.zeros_like(ptab)
    for copy in fetched[:9]:
        copy.wait()

    c1 = spread_of(g1, width, width, g1)
    r2 = spread_of(g2, 2 * width, width, g1)
    r3 = spread_of(g3, 4 * width, width, g1)
    scale_c, shift_c = column(c1, scale_ref[...]), column(c1, shift_ref[...])
    unit_row = iota((g1, 1), 0)
    shift_c = jnp.where((unit_row >= width) & (unit_row < width + 3), ONE, shift_c)
    bias2_c, bias3_c = column(r2, midb_ref[...]), column(r3, outb_ref[...])
    wide1 = hot(spread_of(g1, width, width, g1, True))
    wide2 = hot(spread_of(g2, 2 * width, width, g1, True))
    wide3 = hot(spread_of(g3, 4 * width, width, g1, True))
    mid_t, outer_t = mid_ref[...], outer_ref[...]
    w2 = nn(nt(hot(r2), mid_t).astype(BF16), wide1)
    w2t = nn(nn(hot(c1), mid_t).astype(BF16), wide2)
    w3 = nn(nt(hot(r3), outer_t).astype(BF16), wide2)
    w3t = nn(nn(hot(r2), outer_t).astype(BF16), wide3)
    w2_ref[...] = with_bias(w2, bias2_c, width)
    w3_ref[...] = with_bias(w3, bias3_c, width)
    fold2 = hot(iota((g1, g2), 1) % g1 == iota((g1, g2), 0))
    fold3 = hot(iota((g2, g3), 1) % g2 == iota((g2, g3), 0))
    a2_ref[...] = jnp.concatenate([w2t.astype(BF16), fold2], axis=1)
    a3_ref[...] = jnp.concatenate([w3t.astype(BF16), fold3], axis=1)

    pl.semaphore_wait(barrier, len(found) - 1 + models - 1)
    shares = []
    for slot, off in enumerate(found):
        if off == 0:
            continue
        peer = lax.rem(me + count - off, count)
        for ref, send, recv in ((pos_all, send_a, recv_a), (list_all, send_b, recv_b)):
            copy = pltpu.make_async_remote_copy(
                src_ref=ref.at[0],
                dst_ref=ref.at[slot],
                send_sem=send.at[slot],
                recv_sem=recv.at[slot],
                device_id={"space": peer},
                device_id_type=MESH,
            )
            copy.start()
            shares.append(copy)

    nscr[:, 0:k_total] = nb_ref[...]
    lane = iota((rows, LANES), 1)
    own_row = iota((rows, LANES), 0)
    turned = [
        pltpu.roll(nscr[a * rows : (a + 1) * rows, :], (k_total * a) % LANES, 1) if (k_total * a) % LANES
        else nscr[a * rows : (a + 1) * rows, :]
        for a in range(group)
    ]
    member = []
    wanted = []
    for tile in range(tiles):
        place = lane + tile * LANES
        which = jnp.zeros_like(lane)
        for a in range(1, group):
            which = which + jnp.where(place >= a * k_total, 1, 0)
        member.append(which)
        value = turned[0]
        for a in range(1, group):
            value = jnp.where(which == a, turned[a], value)
        wanted.append(value)

    own_pos = jnp.concatenate([pos_all[0], jnp.zeros((3, LANES - owned), F32)], axis=1)
    for tile in range(tiles):
        at = member[tile] * rows + own_row
        for c in range(3):
            cen_ref[c, :, tile * LANES : (tile + 1) * LANES] = lookup(own_pos[c : c + 1], at)

    fetched[9].wait()

    def order(step, carry):
        source = iota((units * AXIS, 2 * LANES), 0)
        col = iota((units * AXIS, 2 * LANES), 1)
        unit = source >> 4
        padded = unit
        for a in range(1, 4):
            padded = padded + jnp.where(unit >= a * width, g1 - width, 0)
        target = padded + LANES * ((source & (AXIS - 1)) - 2 * step)
        f1p_ref[:, pl.ds(pl.multiple_of(step * 2 * LANES, 2 * LANES), 2 * LANES)] = nn(
            f1_ref[...], hot(target == col)
        ).astype(BF16)
        return carry

    lax.fori_loop(0, AXIS // 2, order, 0)
    sel_ref[...] = hot((iota(sel_ref.shape, 0) >> 7) == iota(sel_ref.shape, 1))

    def own_hot(step, carry):
        for inner in range(ROWS):
            r = step * ROWS + inner
            for tile in range(tiles):
                at = pl.multiple_of((r * tiles + tile) * LANES, LANES)
                which = member[tile][0:1] * rows + r
                oh_ref[LANES : 2 * LANES, pl.ds(at, LANES)] = hot(iota((LANES, LANES), 0) == which)
        return carry

    lax.fori_loop(0, chunks, own_hot, 0)
    for copy in fetched[10:]:
        copy.wait()

    for copy in shares:
        copy.wait_recv()

    base = sum(1 << (16 + 2 * s) for s in range(3))
    where = {off: slot for slot, off in enumerate(found)}

    def neighbour(off, section, side):
        return (off + (-strides[section] if side == 0 else strides[section])) % count

    needs = (
        sorted({(b * strides[1] + c * strides[2]) % count for b in (-1, 0, 1) for c in (-1, 0, 1)}),
        sorted({(c * strides[2]) % count for c in (-1, 0, 1)}),
        [0],
    )
    place = {}
    for section in range(3):
        for off in needs[section]:
            for side in range(2):
                place[(off, 2 * section + side)] = len(place)
    for section in range(3):
        todo = [(off, side) for off in needs[section] for side in range(2)]
        if section == 0:
            for off, side in todo:
                source = neighbour(off, section, side)
                slot = where[source]
                shift = (-1 if side == 0 else 1) << (16 + 2 * section)
                at = place[(off, side)]
                code_ref[at : at + 1, :] = list_all[slot, side] + (slot * owned + base + shift)
            continue
        names, bases, tables = [], [], [[] for _ in range(2 * section)]
        for off, side in todo:
            source = neighbour(off, section, side)
            slot = where[source]
            names.append(list_all[slot, 2 * section + side])
            shift = (-1 if side == 0 else 1) << (16 + 2 * section)
            bases.append((slot * owned + base, shift))
            for block in range(2 * section):
                at = place[(source, block)]
                tables[block].append(code_ref[at : at + 1, :])
        for index, (off, side) in enumerate(todo):
            name = jnp.broadcast_to(names[index], (8, LANES))
            moved = jnp.where(name >= owned, name + (LANES - owned), name)
            row = moved >> 7
            spot = moved & (LANES - 1)
            result = name + bases[index][0]
            for block in range(2 * section):
                result = jnp.where(row == block + 1, lookup(tables[block][index], spot), result)
            at = place[(off, 2 * section + side)]
            code_ref[at : at + 1, :] = result[0:1] + bases[index][1]

    for slot in range(slots):
        at = (slot * owned) % LANES
        ptab[(slot * owned) // LANES, 0:3, at : at + owned] = pos_all[slot]

    for tile in range(tiles):
        cut = slice(tile * LANES, (tile + 1) * LANES)
        j = wanted[tile]
        there = jnp.where(j >= 0, 1.0, 0.0)
        moved = jnp.where(j >= owned, j + (LANES - owned), j)
        row = moved >> 7
        spot = moved & (LANES - 1)
        code = j + base
        for block in range(6):
            at = place[(0, block)]
            code = jnp.where(row == block + 1, lookup(code_ref[at : at + 1, :], spot), code)
        code = jnp.where(j >= 0, code, base)
        ident = code & 65535
        id_ref[tile] = ident
        prow = ident >> 7
        spot = ident & (LANES - 1)
        offs = []
        for c in range(3):
            value = lookup(ptab[0, c : c + 1, :], spot)
            for part in range(1, ptab.shape[0]):
                value = jnp.where(prow == part, lookup(ptab[part, c : c + 1, :], spot), value)
            moved_by = (((code >> (16 + 2 * c)) & 3) - 1).astype(F32)
            offs.append((value + moved_by) - cen_ref[c, :, cut])
        radius = offs[0] * offs[0] + offs[1] * offs[1] + offs[2] * offs[2] + SOFTEN
        inv = lax.rsqrt(radius)
        near = there * inv
        far = near * inv
        there_ref[:, cut] = there
        inv_ref[tile] = inv
        for c in range(4):
            env = near if c == 0 else far * offs[c - 1]
            high = rounded(env)
            low = env - high
            if c > 0:
                off_ref[c - 1, :, cut] = offs[c - 1]
            for twice in range(2):
                e4h_ref[tile, pl.ds(4 * twice + c, rows, stride=8), :] = high
                e4l_ref[tile, pl.ds(4 * twice + c, rows, stride=8), :] = low

    sub8 = iota((8, LANES), 0) >> 2
    picks = [
        [member[tile][0:8] == 2 * v + sub8 for v in range(group // 2)] for tile in range(tiles)
    ]
    w2, w3 = w2_ref[...], w3_ref[...]

    def forward(ch, carry):
        lanes = pl.ds(pl.multiple_of(ch * span, span), span)
        inv = jnp.concatenate(
            [inv_ref[tile, pl.ds(ch * ROWS + inner, 1), :] for inner in range(ROWS) for tile in range(tiles)],
            axis=1,
        )
        t1 = jnp.tanh(scale_c * inv + shift_c)
        t1_ref[:, lanes] = t1
        h1 = t1.astype(BF16)
        h1f = h1.astype(F32)
        u2 = jnp.tanh(nn(w2, h1))
        h2 = (jnp.concatenate([h1f, h1f], axis=0) + u2).astype(BF16)
        s2_ref[:, lanes] = (1.0 - u2 * u2).astype(BF16)
        u3 = jnp.tanh(nn(w3, h2))
        h2f = h2.astype(F32)
        h3 = (jnp.concatenate([h2f, h2f], axis=0) + u3).astype(BF16)
        s3_ref[:, lanes] = (1.0 - u3 * u3).astype(BF16)
        h3_ref[:, lanes] = h3
        for inner in range(ROWS):
            r = ch * ROWS + inner
            for tile in range(tiles):
                cut = slice(tile * LANES, (tile + 1) * LANES)
                at = pl.ds(pl.multiple_of((r * tiles + tile) * LANES, LANES), LANES)
                for part, ref in enumerate((e4h_ref, e4l_ref)):
                    value = ref[tile, pl.ds(pl.multiple_of(r * 8, 8), 8), :]
                    block = jnp.concatenate(
                        [jnp.where(pick, value, 0.0) for pick in picks[tile]], axis=0
                    ).astype(BF16)
                    size = 4 * group
                    em_ref[part * pairs + inner * size : part * pairs + (inner + 1) * size, at] = block
                    if part == 0:
                        em_ref[2 * pairs + inner * size : 2 * pairs + (inner + 1) * size, at] = block
                ident = id_ref[tile, pl.ds(r, 1), :] & (LANES - 1)
                oh_ref[0:LANES, at] = hot(iota((LANES, LANES), 0) == ident)
        moment = nt(em_ref[0 : 2 * pairs, lanes], h3)
        ms_ref[pl.ds(pl.multiple_of(ch * pairs, pairs), pairs), :] = (
            moment[0:pairs] + moment[pairs : 2 * pairs]
        )
        return carry

    lax.fori_loop(0, chunks, forward, 0)

    inverse_k = 1.0 / k_total
    mt = [ms_ref[pl.ds(c, owned, stride=4), :] * inverse_k for c in range(4)]
    for p in range(AXIS):
        total_p = None
        for c in range(4):
            wide = jnp.broadcast_to(mt[c][:, p : p + 1], (owned, LANES))
            bm_ref[c * AXIS + p] = wide
            part = mt[c] * wide
            total_p = part if total_p is None else total_p + part
        d_ref[:, p * LANES : (p + 1) * LANES] = total_p.astype(BF16)

    u1 = jnp.tanh(nt(d_ref[...], f1p_ref[...]) + f1b_ref[...])
    q1 = u1.astype(BF16)
    u2 = jnp.tanh(nt(q1, f2_ref[...]) + f2b_ref[...])
    q2 = (q1.astype(F32) + u2).astype(BF16)
    u3 = jnp.tanh(nt(q2, f3_ref[...]) + f3b_ref[...])
    read = read_ref[...].astype(F32)

    def back(value, weight):
        pair = nn(both(value), weight)
        return rounded(pair[0:owned] + pair[owned : 2 * owned])

    b2 = rounded(read + back(read * ((1.0 + u3) * (1.0 - u3)), f3_ref[...]))
    b1 = rounded(b2 + back(b2 * ((1.0 + u2) * (1.0 - u2)), f2_ref[...]))
    dd_ref[...] = back(b1 * ((1.0 + u1) * (1.0 - u1)), f1p_ref[...])

    sums = [None] * 4
    for p in range(AXIS):
        dd = dd_ref[:, p * LANES : (p + 1) * LANES]
        for c in range(4):
            part = dd * bm_ref[c * AXIS + p]
            sums[c] = part if sums[c] is None else sums[c] + part
            y_ref[c * owned : (c + 1) * owned, p * LANES : (p + 1) * LANES] = (dd * mt[c]).astype(BF16)
    piled = nn(y_ref[...], sel_ref[...])
    for c in range(4):
        dms_ref[pl.ds(c, owned, stride=4), :] = (sums[c] + piled[c * owned : (c + 1) * owned]) * inverse_k

    a2, a3 = a2_ref[...], a3_ref[...]

    def backward(ch, carry):
        lanes = pl.ds(pl.multiple_of(ch * span, span), span)
        high, low = split(dms_ref[pl.ds(pl.multiple_of(ch * pairs, pairs), pairs), :], 2)
        h3 = h3_ref[:, lanes]
        d3 = tn(jnp.concatenate([high, high, low], axis=0), em_ref[:, lanes]).astype(BF16)
        p3 = d3 * s3_ref[:, lanes]
        d2 = nn(a3, jnp.concatenate([p3, d3], axis=0)).astype(BF16)
        p2 = d2 * s2_ref[:, lanes]
        d1 = nn(a2, jnp.concatenate([p2, d2], axis=0))
        t1 = t1_ref[:, lanes]
        p1 = jnp.sum(d1 * (1.0 - t1 * t1) * scale_c, axis=0, keepdims=True)
        denv = nn(jnp.concatenate([high, low], axis=0), h3)
        denv = denv[0:pairs] + denv[pairs : 2 * pairs]
        for inner in range(ROWS):
            r = ch * ROWS + inner
            for tile in range(tiles):
                at = (inner * tiles + tile) * LANES
                di_ref[tile, pl.ds(r, 1), :] = p1[:, at : at + LANES]
                value = None
                for v, pick in enumerate(picks[tile]):
                    first = inner * 4 * group + 8 * v
                    part = jnp.where(pick, denv[first : first + 8, at : at + LANES], 0.0)
                    value = part if value is None else value + part
                value = value + pltpu.roll(value, 4, 0)
                de4_ref[tile, pl.ds(pl.multiple_of(r * 8, 8), 8), :] = value
        return carry

    lax.fori_loop(0, chunks, backward, 0)

    for tile in range(tiles):
        cut = slice(tile * LANES, (tile + 1) * LANES)
        offs = [off_ref[a, :, cut] for a in range(3)]
        inv, there = inv_ref[tile], there_ref[:, cut]
        denv = [de4_ref[tile, pl.ds(c, rows, stride=8), :] for c in range(4)]
        near = there * inv
        far = near * inv
        mixed = denv[1] * offs[0] + denv[2] * offs[1] + denv[3] * offs[2]
        dinv = di_ref[tile] + there * denv[0] + 2.0 * near * mixed
        pull = dinv * (inv * inv * inv)
        grads = [far * denv[a + 1] - pull * offs[a] for a in range(3)]
        terms = [-one for one in grads]
        terms += [-(offs[a] * grads[b]) for a in range(3) for b in range(3)]
        for at, term in enumerate(terms):
            high = rounded(term)
            th_ref[tile, pl.ds(at, rows, stride=16), :] = high
            tl_ref[tile, pl.ds(at, rows, stride=16), :] = term - high

    def scatter(ch, sums):
        for inner in range(ROWS):
            r = ch * ROWS + inner
            for tile in range(tiles):
                cut = slice(tile * LANES, (tile + 1) * LANES)
                at = slice((inner * tiles + tile) * LANES, (inner * tiles + tile + 1) * LANES)
                band = jnp.broadcast_to(id_ref[tile, pl.ds(r, 1), :] >> 7, (16, LANES))
                for part, ref in enumerate((th_ref, tl_ref)):
                    value = ref[tile, pl.ds(pl.multiple_of(r * 16, 16), 16), :]
                    for m in range(masks_count):
                        first = (2 * m + part) * 16
                        lhs_ref[first : first + 16, at] = jnp.where(band == m, value, 0.0).astype(BF16)
        lanes = pl.ds(pl.multiple_of(ch * span, span), span)
        return sums + nt(lhs_ref[...], oh_ref[:, lanes])

    sums = lax.fori_loop(0, chunks, scatter, jnp.zeros((32 * masks_count, 2 * LANES), F32))
    centre = jnp.zeros((16, LANES), F32)
    for m in range(masks_count):
        upper = sums[32 * m : 32 * m + 16]
        lower = sums[32 * m + 16 : 32 * m + 32]
        whole = upper + lower
        part_ref[m] = whole[:, 0:LANES]
        centre = centre + whole[:, LANES : 2 * LANES]
    centre = jnp.where(iota((16, LANES), 0) < 3, centre, 0.0)
    mine = part_ref[0] - centre

    sent = []
    for slot, off in enumerate(found):
        if off == 0:
            continue
        copy = pltpu.make_async_remote_copy(
            src_ref=part_ref.at[(slot * owned) // LANES],
            dst_ref=held.at[slot],
            send_sem=send_c.at[slot],
            recv_sem=recv_c.at[slot],
            device_id={"space": lax.rem(me + off, count)},
            device_id_type=MESH,
        )
        copy.start()
        sent.append(copy)
    for copy in sent:
        copy.wait_recv()
    per = LANES // owned
    lots = [None] * per
    for slot in range(slots):
        value = mine if slot == 0 else held[slot]
        lots[slot % per] = value if lots[slot % per] is None else lots[slot % per] + value
    own = lots[0]
    for at in range(1, per):
        own = own + pltpu.roll(lots[at], LANES - at * owned, 1)
    total[...] = own
    last = []
    for step in range(1, models):
        copy = pltpu.make_async_remote_copy(
            src_ref=total,
            dst_ref=others.at[step],
            send_sem=send_d.at[step],
            recv_sem=recv_d.at[step],
            device_id={"mp": lax.rem(model + step, models)},
            device_id_type=MESH,
        )
        copy.start()
        last.append(copy)
    for copy in shares + sent:
        copy.wait_send()
    for copy in last:
        copy.wait_recv()
    stacked = [own] + [others[step] for step in range(1, models)]
    mean = sum(stacked[1:], stacked[0]) * (1.0 / models)
    square = jnp.zeros_like(mean)
    for one in stacked:
        square = square + (one - mean) * (one - mean)
    square = square * (1.0 / models)
    row = iota(square.shape, 0)
    force = jnp.sum(jnp.where(row < 3, square, 0.0), axis=0, keepdims=True)
    virial = jnp.sum(jnp.where((row >= 3) & (row < 12), square, 0.0), axis=0, keepdims=True)
    quarter = owned // models

    def pick_mine(value):
        result = value[:, 0:quarter]
        for part in range(1, models):
            result = jnp.where(model == part, value[:, part * quarter : (part + 1) * quarter], result)
        return result

    means = pick_mine(mean[0:3])
    for c in range(3):
        mean_ref[c, 0] = means[c : c + 1]
    force_ref[0] = pick_mine(force)
    virial_ref[0] = pick_mine(virial)
    for copy in last:
        copy.wait_send()


def local(positions, send_lists, neighbours, *weights):
    count = lax.axis_size("space")
    models = lax.axis_size("mp")
    strides, found = dims(count)
    slots = len(found)
    owned = positions.shape[1]
    k_total = neighbours.shape[0]
    width = weights[0].shape[1]
    units = 4 * width
    quarter = owned // models
    blocks, cap = send_lists.shape[1:]
    lists = jnp.transpose(send_lists, (1, 0, 2))
    named = neighbours.T
    scale, shift, mid, midb, outer, outb, f1, f1b, f2, f2b, f3, f3b, read = weights
    mid = jnp.swapaxes(mid, 1, 2)
    outer = jnp.swapaxes(outer, 1, 2)
    fit = f1.shape[1]
    group = LANES // math.gcd(k_total, LANES)
    rows = owned // group
    all_pairs = owned * k_total
    row_lanes = group * k_total
    tiles = row_lanes // LANES
    pairs = ROWS * group * 4
    bands = (slots * owned + LANES - 1) // LANES
    span = ROWS * row_lanes
    args = (positions, lists, named, scale, shift, mid, midb, outer, outb, f1, f1b, f2, f2b, f3, f3b, read)

    def vm(shape, dtype=F32):
        return pltpu.VMEM(shape, dtype)

    scratch = [
        vm((slots, 3, owned)), vm((slots, blocks, 1, cap), I32), vm((owned, k_total), I32),
        vm((1, width)), vm((1, width)), vm((width, 2 * width), BF16), vm((1, 2 * width)),
        vm((2 * width, 4 * width), BF16), vm((1, 4 * width)),
        vm((fit, units * AXIS), BF16), vm((1, fit)), vm((fit, fit), BF16), vm((1, fit)),
        vm((fit, fit), BF16), vm((1, fit)), vm((1, fit), BF16),
        vm((owned, LANES), I32), vm((bands, 8, LANES)), vm((64, LANES), I32),
        vm((fit, AXIS * LANES), BF16), vm((AXIS * LANES, LANES), BF16),
        vm((2 * LANES, all_pairs), BF16), vm((3 * pairs, all_pairs), BF16),
        vm((64, 32), BF16), vm((128, 64), BF16), vm((32, 128), BF16), vm((64, 256), BF16),
        vm((3, rows, row_lanes)), vm((tiles, rows, LANES)), vm((rows, row_lanes)),
        vm((tiles, rows, LANES), I32), vm((3, rows, row_lanes)),
        vm((tiles, 8 * rows, LANES)), vm((tiles, 8 * rows, LANES)),
        vm((32, all_pairs)), vm((64, all_pairs), BF16), vm((128, all_pairs), BF16),
        vm((128, all_pairs), BF16), vm((4 * owned, LANES)), vm((4 * AXIS, owned, LANES)),
        vm((owned, AXIS * LANES), BF16), vm((owned, AXIS * LANES)),
        vm((4 * owned, AXIS * LANES), BF16), vm((4 * owned, LANES)),
        vm((tiles, 8 * rows, LANES)), vm((tiles, rows, LANES)),
        vm((tiles, 16 * rows, LANES)), vm((tiles, 16 * rows, LANES)), vm((32 * bands, span), BF16),
        vm((bands, 16, LANES)), vm((slots, 16, LANES)), vm((16, LANES)), vm((models, 16, LANES)),
        pltpu.SemaphoreType.DMA((len(args),)),
    ]
    scratch += [pltpu.SemaphoreType.DMA((slots,))] * 6 + [pltpu.SemaphoreType.DMA((models,))] * 2
    return pl.pallas_call(
        functools.partial(
            kernel, count, models, strides, found, (owned, k_total, width, fit)
        ),
        out_shape=(
            jax.ShapeDtypeStruct((3, 1, 1, quarter), F32),
            jax.ShapeDtypeStruct((1, 1, quarter), F32),
            jax.ShapeDtypeStruct((1, 1, quarter), F32),
        ),
        in_specs=[ANY] * len(args),
        out_specs=(VM, VM, VM),
        scratch_shapes=scratch,
        compiler_params=pltpu.CompilerParams(
            collective_id=0, has_side_effects=True, vmem_limit_bytes=60000000
        ),
        name="forces",
    )(*args)


def solution(mesh):
    flat, deep = P("mp", None), P("mp", None, None)
    return jax.shard_map(
        local,
        mesh=mesh,
        in_specs=(
            P(None, "space"), P("space", None, None), P(None, "space"),
            flat, flat, deep, flat, deep, flat, deep, flat, deep, flat, deep, flat, flat,
        ),
        out_specs=(P(None, "space", "mp", None), P("space", "mp", None), P("space", "mp", None)),
        check_vma=False,
    )
```

```python
import functools
import math

import jax
import jax.numpy as jnp
from jax import lax
from jax.experimental import pallas as pl
from jax.experimental.pallas import tpu as pltpu
from jax.sharding import PartitionSpec as P

AXIS = 16
SOFTEN = 0.04
LANES = 128
ROWS = 2
ONE = 20.0
MESH = pl.DeviceIdType.MESH
F32 = jnp.float32
BF16 = jnp.bfloat16
I32 = jnp.int32
ANY = pl.BlockSpec(memory_space=pl.ANY)
VM = pl.BlockSpec(memory_space=pltpu.VMEM)


def dims(space_count):
    grid_y = min(4, max(2, space_count // 16))
    strides = (grid_y * grid_y, grid_y, 1)
    span = (-1, 0, 1)
    found = sorted(
        {
            (a * strides[0] + b * strides[1] + c * strides[2]) % space_count
            for a in span
            for b in span
            for c in span
        }
    )
    return strides, found


def nn(a, b):
    return jnp.dot(a, b, preferred_element_type=F32)


def nt(a, b):
    return lax.dot_general(a, b, (((1,), (1,)), ((), ())), preferred_element_type=F32)


def tn(a, b):
    return lax.dot_general(a, b, (((0,), (0,)), ((), ())), preferred_element_type=F32)


def iota(shape, dim):
    return lax.broadcasted_iota(I32, shape, dim)


def hot(mask):
    return jnp.where(mask, 1.0, 0.0).astype(BF16)


def spread_of(rows, units, width, group, flip=False):
    shape = (units, rows) if flip else (rows, units)
    row = iota(shape, 1 if flip else 0)
    unit = iota(shape, 0 if flip else 1)
    inner = row % group
    return (inner < width) & (unit == (row // group) * width + inner)


def column(mask, row_value):
    return jnp.sum(jnp.where(mask, row_value, 0.0), axis=1, keepdims=True)


def rounded(value):
    return value.astype(BF16).astype(F32)


def split(value, parts):
    pieces = []
    for _ in range(parts):
        piece = value.astype(BF16)
        pieces.append(piece)
        value = value - piece.astype(F32)
    return pieces


def both(value):
    return jnp.concatenate(split(value, 2), axis=0)


def lookup(row, lane):
    return jnp.take_along_axis(
        jnp.broadcast_to(row, lane.shape), lane, axis=1, mode="promise_in_bounds"
    )


def with_bias(weight, bias, width):
    col = iota(weight.shape, 1)
    for place, piece in enumerate(split(bias, 3)):
        weight = jnp.where(col == width + place, piece.astype(F32), weight)
    return weight.astype(BF16)


def kernel(
    count, models, strides, found, sizes,
    pos_in, list_in, nb_in,
    scale_in, shift_in, mid_in, midb_in, outer_in, outb_in,
    f1_in, f1b_in, f2_in, f2b_in, f3_in, f3b_in, read_in,
    mean_ref, force_ref, virial_ref,
    pos_all, list_all, nb_ref, scale_ref, shift_ref, mid_ref, midb_ref, outer_ref, outb_ref,
    f1_ref, f1b_ref, f2_ref, f2b_ref, f3_ref, f3b_ref, read_ref,
    nscr, ptab, code_ref, to_ref, f1p_ref, sel_ref, oh_ref, em_ref,
    w2_ref, w3_ref, a2_ref, a3_ref,
    off_ref, inv_ref, there_ref, id_ref, cen_ref, e4h_ref, e4l_ref,
    t1_ref, s2_ref, s3_ref, h3_ref, ms_ref, bm_ref, d_ref, dd_ref, y_ref, dms_ref,
    de4_ref, di_ref, th_ref, tl_ref, lhs_ref, part_ref, held, total, others,
    local_sem, send_a, recv_a, send_b, recv_b, send_c, recv_c, send_d, recv_d,
):
    owned, k_total, width, fit = sizes
    slots = len(found)
    group = LANES // math.gcd(k_total, LANES)
    tiles = group * k_total // LANES
    rows = owned // group
    chunks = rows // ROWS
    span = ROWS * tiles * LANES
    units = 4 * width
    g1, g2, g3 = 32, 64, 128
    pairs = ROWS * group * 4
    masks_count = (slots * owned + LANES - 1) // LANES
    me = lax.axis_index("space")
    model = lax.axis_index("mp")

    barrier = pltpu.get_barrier_semaphore()
    for off in found[1:]:
        pl.semaphore_signal(
            barrier, inc=1, device_id={"space": lax.rem(me + off, count)}, device_id_type=MESH
        )
    for step in range(1, models):
        pl.semaphore_signal(
            barrier, inc=1, device_id={"mp": lax.rem(model + step, models)}, device_id_type=MESH
        )
    moves = [
        (pos_in, pos_all.at[0]), (list_in, list_all.at[0]), (nb_in, nb_ref),
        (scale_in, scale_ref), (shift_in, shift_ref), (mid_in.at[0], mid_ref), (midb_in, midb_ref),
        (outer_in.at[0], outer_ref), (outb_in, outb_ref), (f1_in.at[0], f1_ref), (f1b_in, f1b_ref),
        (f2_in.at[0], f2_ref), (f2b_in, f2b_ref), (f3_in.at[0], f3_ref), (f3b_in, f3b_ref),
        (read_in, read_ref),
    ]
    fetched = []
    for place, (src, dst) in enumerate(moves):
        copy = pltpu.make_async_copy(src, dst, local_sem.at[place])
        copy.start()
        fetched.append(copy)
    for copy in fetched[:2]:
        copy.wait()
    pl.semaphore_wait(barrier, len(found) - 1 + models - 1)
    shares = []
    for slot, off in enumerate(found):
        if off == 0:
            continue
        peer = lax.rem(me + count - off, count)
        for ref, send, recv in ((pos_all, send_a, recv_a), (list_all, send_b, recv_b)):
            copy = pltpu.make_async_remote_copy(
                src_ref=ref.at[0],
                dst_ref=ref.at[slot],
                send_sem=send.at[slot],
                recv_sem=recv.at[slot],
                device_id={"space": peer},
                device_id_type=MESH,
            )
            copy.start()
            shares.append(copy)

    em_ref[...] = jnp.zeros_like(em_ref)
    th_ref[...] = jnp.zeros_like(th_ref)
    tl_ref[...] = jnp.zeros_like(tl_ref)
    nscr[...] = jnp.zeros_like(nscr)
    ptab[...] = jnp.zeros_like(ptab)
    for copy in fetched[2:9]:
        copy.wait()
    c1 = spread_of(g1, width, width, g1)
    r2 = spread_of(g2, 2 * width, width, g1)
    r3 = spread_of(g3, 4 * width, width, g1)
    scale_c, shift_c = column(c1, scale_ref[...]), column(c1, shift_ref[...])
    unit_row = iota((g1, 1), 0)
    shift_c = jnp.where((unit_row >= width) & (unit_row < width + 3), ONE, shift_c)
    bias2_c, bias3_c = column(r2, midb_ref[...]), column(r3, outb_ref[...])
    wide1 = hot(spread_of(g1, width, width, g1, True))
    wide2 = hot(spread_of(g2, 2 * width, width, g1, True))
    wide3 = hot(spread_of(g3, 4 * width, width, g1, True))
    mid_t, outer_t = mid_ref[...], outer_ref[...]
    w2 = nn(nt(hot(r2), mid_t).astype(BF16), wide1)
    w2t = nn(nn(hot(c1), mid_t).astype(BF16), wide2)
    w3 = nn(nt(hot(r3), outer_t).astype(BF16), wide2)
    w3t = nn(nn(hot(r2), outer_t).astype(BF16), wide3)
    w2_ref[...] = with_bias(w2, bias2_c, width)
    w3_ref[...] = with_bias(w3, bias3_c, width)
    fold2 = hot(iota((g1, g2), 1) % g1 == iota((g1, g2), 0))
    fold3 = hot(iota((g2, g3), 1) % g2 == iota((g2, g3), 0))
    a2_ref[...] = jnp.concatenate([w2t.astype(BF16), fold2], axis=1)
    a3_ref[...] = jnp.concatenate([w3t.astype(BF16), fold3], axis=1)

    nscr[:, 0:k_total] = nb_ref[...]
    lane = iota((rows, LANES), 1)
    own_row = iota((rows, LANES), 0)
    turned = [
        pltpu.roll(nscr[a * rows : (a + 1) * rows, :], (k_total * a) % LANES, 1) if (k_total * a) % LANES
        else nscr[a * rows : (a + 1) * rows, :]
        for a in range(group)
    ]
    member = []
    wanted = []
    for tile in range(tiles):
        place = lane + tile * LANES
        which = jnp.zeros_like(lane)
        for a in range(1, group):
            which = which + jnp.where(place >= a * k_total, 1, 0)
        member.append(which)
        value = turned[0]
        for a in range(1, group):
            value = jnp.where(which == a, turned[a], value)
        wanted.append(value)

    own_pos = jnp.concatenate([pos_all[0], jnp.zeros((3, LANES - owned), F32)], axis=1)
    for tile in range(tiles):
        at = member[tile] * rows + own_row
        for c in range(3):
            cen_ref[c, :, tile * LANES : (tile + 1) * LANES] = lookup(own_pos[c : c + 1], at)

    fetched[9].wait()

    source = iota((units * AXIS, LANES), 0)
    unit = source >> 4
    padded = unit
    for a in range(1, 4):
        padded = padded + jnp.where(unit >= a * width, g1 - width, 0)
    to_ref[...] = padded + LANES * (source & (AXIS - 1)) - iota((units * AXIS, LANES), 1)

    def order(step):
        target = to_ref[...]
        pick = jnp.concatenate(
            [hot(target == LANES * (2 * step)), hot(target == LANES * (2 * step + 1))], axis=1
        )
        f1p_ref[:, pl.ds(pl.multiple_of(step * 2 * LANES, 2 * LANES), 2 * LANES)] = nn(
            f1_ref[...], pick
        ).astype(BF16)

    for step in range(AXIS // 2):
        order(step)
    sel_ref[...] = hot((iota(sel_ref.shape, 0) >> 7) == iota(sel_ref.shape, 1))

    def own_hot(step):
        for inner in range(ROWS):
            r = step * ROWS + inner
            for tile in range(tiles):
                at = slice((inner * tiles + tile) * LANES, (inner * tiles + tile + 1) * LANES)
                which = member[tile][0:1] * rows + r
                oh_ref[step, LANES : 2 * LANES, at] = hot(iota((LANES, LANES), 0) == which)

    for step in range(chunks):
        own_hot(step)
    for copy in fetched[10:]:
        copy.wait()

    for copy in shares:
        copy.wait_recv()

    base = sum(1 << (16 + 2 * s) for s in range(3))
    where = {off: slot for slot, off in enumerate(found)}

    def neighbour(off, section, side):
        return (off + (-strides[section] if side == 0 else strides[section])) % count

    needs = (
        sorted({(b * strides[1] + c * strides[2]) % count for b in (-1, 0, 1) for c in (-1, 0, 1)}),
        sorted({(c * strides[2]) % count for c in (-1, 0, 1)}),
        [0],
    )
    place = {}
    for section in range(3):
        for off in needs[section]:
            for side in range(2):
                place[(off, 2 * section + side)] = len(place)
    for section in range(3):
        todo = [(off, side) for off in needs[section] for side in range(2)]
        if section == 0:
            for off, side in todo:
                source = neighbour(off, section, side)
                slot = where[source]
                shift = (-1 if side == 0 else 1) << (16 + 2 * section)
                at = place[(off, side)]
                code_ref[at : at + 1, :] = list_all[slot, side] + (slot * owned + base + shift)
            continue
        names, bases, tables = [], [], [[] for _ in range(2 * section)]
        for off, side in todo:
            source = neighbour(off, section, side)
            slot = where[source]
            names.append(list_all[slot, 2 * section + side])
            shift = (-1 if side == 0 else 1) << (16 + 2 * section)
            bases.append((slot * owned + base, shift))
            for block in range(2 * section):
                at = place[(source, block)]
                tables[block].append(code_ref[at : at + 1, :])
        for index, (off, side) in enumerate(todo):
            name = jnp.broadcast_to(names[index], (8, LANES))
            moved = jnp.where(name >= owned, name + (LANES - owned), name)
            row = moved >> 7
            spot = moved & (LANES - 1)
            result = name + bases[index][0]
            for block in range(2 * section):
                result = jnp.where(row == block + 1, lookup(tables[block][index], spot), result)
            at = place[(off, 2 * section + side)]
            code_ref[at : at + 1, :] = result[0:1] + bases[index][1]

    for slot in range(slots):
        at = (slot * owned) % LANES
        ptab[(slot * owned) // LANES, 0:3, at : at + owned] = pos_all[slot]

    for tile in range(tiles):
        cut = slice(tile * LANES, (tile + 1) * LANES)
        j = wanted[tile]
        there = jnp.where(j >= 0, 1.0, 0.0)
        moved = jnp.where(j >= owned, j + (LANES - owned), j)
        row = moved >> 7
        spot = moved & (LANES - 1)
        code = j + base
        for block in range(6):
            at = place[(0, block)]
            code = jnp.where(row == block + 1, lookup(code_ref[at : at + 1, :], spot), code)
        code = jnp.where(j >= 0, code, base)
        ident = code & 65535
        id_ref[tile] = ident
        prow = ident >> 7
        spot = ident & (LANES - 1)
        offs = []
        for c in range(3):
            value = lookup(ptab[0, c : c + 1, :], spot)
            for part in range(1, ptab.shape[0]):
                value = jnp.where(prow == part, lookup(ptab[part, c : c + 1, :], spot), value)
            moved_by = (((code >> (16 + 2 * c)) & 3) - 1).astype(F32)
            offs.append((value + moved_by) - cen_ref[c, :, cut])
        radius = offs[0] * offs[0] + offs[1] * offs[1] + offs[2] * offs[2] + SOFTEN
        inv = lax.rsqrt(radius)
        near = there * inv
        far = near * inv
        there_ref[:, cut] = there
        inv_ref[tile] = inv
        for c in range(4):
            env = near if c == 0 else far * offs[c - 1]
            high = rounded(env)
            low = env - high
            if c > 0:
                off_ref[c - 1, :, cut] = offs[c - 1]
            for twice in range(2):
                e4h_ref[tile, pl.ds(4 * twice + c, rows, stride=8), :] = high
                e4l_ref[tile, pl.ds(4 * twice + c, rows, stride=8), :] = low

    sub8 = iota((8, LANES), 0) >> 2
    picks = [
        [member[tile][0:8] == 2 * v + sub8 for v in range(group // 2)] for tile in range(tiles)
    ]
    w2, w3 = w2_ref[...], w3_ref[...]

    def forward(ch):
        inv = jnp.concatenate(
            [inv_ref[tile, pl.ds(ch * ROWS + inner, 1), :] for inner in range(ROWS) for tile in range(tiles)],
            axis=1,
        )
        t1 = jnp.tanh(scale_c * inv + shift_c)
        t1_ref[ch] = t1
        h1 = t1.astype(BF16)
        h1f = h1.astype(F32)
        u2 = jnp.tanh(nn(w2, h1))
        h2 = (jnp.concatenate([h1f, h1f], axis=0) + u2).astype(BF16)
        s2_ref[ch] = (1.0 - u2 * u2).astype(BF16)
        u3 = jnp.tanh(nn(w3, h2))
        h2f = h2.astype(F32)
        h3 = (jnp.concatenate([h2f, h2f], axis=0) + u3).astype(BF16)
        s3_ref[ch] = (1.0 - u3 * u3).astype(BF16)
        h3_ref[ch] = h3
        for inner in range(ROWS):
            r = ch * ROWS + inner
            for tile in range(tiles):
                cut = slice(tile * LANES, (tile + 1) * LANES)
                at = slice((inner * tiles + tile) * LANES, (inner * tiles + tile + 1) * LANES)
                for part, ref in enumerate((e4h_ref, e4l_ref)):
                    value = ref[tile, pl.ds(pl.multiple_of(r * 8, 8), 8), :]
                    block = jnp.concatenate(
                        [jnp.where(pick, value, 0.0) for pick in picks[tile]], axis=0
                    ).astype(BF16)
                    size = 4 * group
                    em_ref[ch, part * pairs + inner * size : part * pairs + (inner + 1) * size, at] = block
                    if part == 0:
                        em_ref[ch, 2 * pairs + inner * size : 2 * pairs + (inner + 1) * size, at] = block
                ident = id_ref[tile, pl.ds(r, 1), :] & (LANES - 1)
                oh_ref[ch, 0:LANES, at] = hot(iota((LANES, LANES), 0) == ident)
        moment = nt(em_ref[ch, 0 : 2 * pairs, :], h3)
        ms_ref[pl.ds(pl.multiple_of(ch * pairs, pairs), pairs), :] = (
            moment[0:pairs] + moment[pairs : 2 * pairs]
        )

    for ch in range(chunks):
        forward(ch)

    inverse_k = 1.0 / k_total
    mt = [ms_ref[pl.ds(c, owned, stride=4), :] * inverse_k for c in range(4)]
    for p in range(AXIS):
        total_p = None
        for c in range(4):
            wide = jnp.broadcast_to(mt[c][:, p : p + 1], (owned, LANES))
            bm_ref[c * AXIS + p] = wide
            part = mt[c] * wide
            total_p = part if total_p is None else total_p + part
        d_ref[:, p * LANES : (p + 1) * LANES] = total_p.astype(BF16)

    u1 = jnp.tanh(nt(d_ref[...], f1p_ref[...]) + f1b_ref[...])
    q1 = u1.astype(BF16)
    u2 = jnp.tanh(nt(q1, f2_ref[...]) + f2b_ref[...])
    q2 = (q1.astype(F32) + u2).astype(BF16)
    u3 = jnp.tanh(nt(q2, f3_ref[...]) + f3b_ref[...])
    read = read_ref[...].astype(F32)

    def back(value, weight):
        pair = nn(both(value), weight)
        return rounded(pair[0:owned] + pair[owned : 2 * owned])

    b2 = read + back(read * ((1.0 + u3) * (1.0 - u3)), f3_ref[...])
    b1 = rounded(b2) + back(b2 * ((1.0 + u2) * (1.0 - u2)), f2_ref[...])
    dd_ref[...] = back(b1 * ((1.0 + u1) * (1.0 - u1)), f1p_ref[...])

    sums = [None] * 4
    for p in range(AXIS):
        dd = dd_ref[:, p * LANES : (p + 1) * LANES]
        for c in range(4):
            part = dd * bm_ref[c * AXIS + p]
            sums[c] = part if sums[c] is None else sums[c] + part
            y_ref[c * owned : (c + 1) * owned, p * LANES : (p + 1) * LANES] = (dd * mt[c]).astype(BF16)
    piled = nn(y_ref[...], sel_ref[...])
    for c in range(4):
        dms_ref[pl.ds(c, owned, stride=4), :] = (sums[c] + piled[c * owned : (c + 1) * owned]) * inverse_k

    a2, a3 = a2_ref[...], a3_ref[...]

    def backward(ch):
        high, low = split(dms_ref[pl.ds(pl.multiple_of(ch * pairs, pairs), pairs), :], 2)
        h3 = h3_ref[ch]
        d3 = tn(jnp.concatenate([high, high, low], axis=0), em_ref[ch]).astype(BF16)
        p3 = d3 * s3_ref[ch]
        d2 = nn(a3, jnp.concatenate([p3, d3], axis=0)).astype(BF16)
        p2 = d2 * s2_ref[ch]
        d1 = nn(a2, jnp.concatenate([p2, d2], axis=0))
        t1 = t1_ref[ch]
        p1 = jnp.sum(d1 * (1.0 - t1 * t1) * scale_c, axis=0, keepdims=True)
        denv = nn(jnp.concatenate([high, low], axis=0), h3)
        denv = denv[0:pairs] + denv[pairs : 2 * pairs]
        for inner in range(ROWS):
            r = ch * ROWS + inner
            for tile in range(tiles):
                at = (inner * tiles + tile) * LANES
                di_ref[tile, pl.ds(r, 1), :] = p1[:, at : at + LANES]
                value = None
                for v, pick in enumerate(picks[tile]):
                    first = inner * 4 * group + 8 * v
                    part = jnp.where(pick, denv[first : first + 8, at : at + LANES], 0.0)
                    value = part if value is None else value + part
                value = value + pltpu.roll(value, 4, 0)
                de4_ref[tile, pl.ds(pl.multiple_of(r * 8, 8), 8), :] = value

    for ch in range(chunks):
        backward(ch)

    for tile in range(tiles):
        cut = slice(tile * LANES, (tile + 1) * LANES)
        offs = [off_ref[a, :, cut] for a in range(3)]
        inv, there = inv_ref[tile], there_ref[:, cut]
        denv = [de4_ref[tile, pl.ds(c, rows, stride=8), :] for c in range(4)]
        near = there * inv
        far = near * inv
        mixed = denv[1] * offs[0] + denv[2] * offs[1] + denv[3] * offs[2]
        dinv = di_ref[tile] + there * denv[0] + 2.0 * near * mixed
        pull = dinv * (inv * inv * inv)
        grads = [far * denv[a + 1] - pull * offs[a] for a in range(3)]
        terms = [-one for one in grads]
        terms += [-(offs[a] * grads[b]) for a in range(3) for b in range(3)]
        for at, term in enumerate(terms):
            high = rounded(term)
            th_ref[tile, pl.ds(at, rows, stride=16), :] = high
            tl_ref[tile, pl.ds(at, rows, stride=16), :] = term - high

    def scatter(ch, sums):
        for inner in range(ROWS):
            r = ch * ROWS + inner
            for tile in range(tiles):
                cut = slice(tile * LANES, (tile + 1) * LANES)
                at = slice((inner * tiles + tile) * LANES, (inner * tiles + tile + 1) * LANES)
                band = jnp.broadcast_to(id_ref[tile, pl.ds(r, 1), :] >> 7, (16, LANES))
                for part, ref in enumerate((th_ref, tl_ref)):
                    value = ref[tile, pl.ds(pl.multiple_of(r * 16, 16), 16), :]
                    for m in range(masks_count):
                        first = (2 * m + part) * 16
                        lhs_ref[first : first + 16, at] = jnp.where(band == m, value, 0.0).astype(BF16)
        return sums + nt(lhs_ref[...], oh_ref[ch])

    sums = jnp.zeros((32 * masks_count, 2 * LANES), F32)
    for ch in range(chunks):
        sums = scatter(ch, sums)
    centre = jnp.zeros((16, LANES), F32)
    for m in range(masks_count):
        upper = sums[32 * m : 32 * m + 16]
        lower = sums[32 * m + 16 : 32 * m + 32]
        whole = upper + lower
        part_ref[m] = whole[:, 0:LANES]
        centre = centre + whole[:, LANES : 2 * LANES]
    centre = jnp.where(iota((16, LANES), 0) < 3, centre, 0.0)
    mine = part_ref[0] - centre

    sent = []
    for slot, off in enumerate(found):
        if off == 0:
            continue
        copy = pltpu.make_async_remote_copy(
            src_ref=part_ref.at[(slot * owned) // LANES],
            dst_ref=held.at[slot],
            send_sem=send_c.at[slot],
            recv_sem=recv_c.at[slot],
            device_id={"space": lax.rem(me + off, count)},
            device_id_type=MESH,
        )
        copy.start()
        sent.append(copy)
    for copy in sent:
        copy.wait_recv()
    per = LANES // owned
    lots = [None] * per
    for slot in range(slots):
        value = mine if slot == 0 else held[slot]
        lots[slot % per] = value if lots[slot % per] is None else lots[slot % per] + value
    own = lots[0]
    for at in range(1, per):
        own = own + pltpu.roll(lots[at], LANES - at * owned, 1)
    total[...] = own
    last = []
    for step in range(1, models):
        copy = pltpu.make_async_remote_copy(
            src_ref=total,
            dst_ref=others.at[step],
            send_sem=send_d.at[step],
            recv_sem=recv_d.at[step],
            device_id={"mp": lax.rem(model + step, models)},
            device_id_type=MESH,
        )
        copy.start()
        last.append(copy)
    for copy in shares + sent:
        copy.wait_send()
    for copy in last:
        copy.wait_recv()
    stacked = [own] + [others[step] for step in range(1, models)]
    mean = sum(stacked[1:], stacked[0]) * (1.0 / models)
    square = jnp.zeros_like(mean)
    for one in stacked:
        square = square + (one - mean) * (one - mean)
    square = square * (1.0 / models)
    row = iota(square.shape, 0)
    force = jnp.sum(jnp.where(row < 3, square, 0.0), axis=0, keepdims=True)
    virial = jnp.sum(jnp.where((row >= 3) & (row < 12), square, 0.0), axis=0, keepdims=True)
    quarter = owned // models

    def pick_mine(value):
        result = value[:, 0:quarter]
        for part in range(1, models):
            result = jnp.where(model == part, value[:, part * quarter : (part + 1) * quarter], result)
        return result

    means = pick_mine(mean[0:3])
    for c in range(3):
        mean_ref[c, 0] = means[c : c + 1]
    force_ref[0] = pick_mine(force)
    virial_ref[0] = pick_mine(virial)
    for copy in last:
        copy.wait_send()


def local(positions, send_lists, neighbours, *weights):
    count = lax.axis_size("space")
    models = lax.axis_size("mp")
    strides, found = dims(count)
    slots = len(found)
    owned = positions.shape[1]
    k_total = neighbours.shape[0]
    width = weights[0].shape[1]
    units = 4 * width
    quarter = owned // models
    blocks, cap = send_lists.shape[1:]
    lists = jnp.transpose(send_lists, (1, 0, 2))
    named = neighbours.T
    scale, shift, mid, midb, outer, outb, f1, f1b, f2, f2b, f3, f3b, read = weights
    mid = jnp.swapaxes(mid, 1, 2)
    outer = jnp.swapaxes(outer, 1, 2)
    fit = f1.shape[1]
    group = LANES // math.gcd(k_total, LANES)
    rows = owned // group
    row_lanes = group * k_total
    tiles = row_lanes // LANES
    pairs = ROWS * group * 4
    bands = (slots * owned + LANES - 1) // LANES
    span = ROWS * row_lanes
    chunks = rows // ROWS
    args = (positions, lists, named, scale, shift, mid, midb, outer, outb, f1, f1b, f2, f2b, f3, f3b, read)

    def vm(shape, dtype=F32):
        return pltpu.VMEM(shape, dtype)

    scratch = [
        vm((slots, 3, owned)), vm((slots, blocks, 1, cap), I32), vm((owned, k_total), I32),
        vm((1, width)), vm((1, width)), vm((width, 2 * width), BF16), vm((1, 2 * width)),
        vm((2 * width, 4 * width), BF16), vm((1, 4 * width)),
        vm((fit, units * AXIS), BF16), vm((1, fit)), vm((fit, fit), BF16), vm((1, fit)),
        vm((fit, fit), BF16), vm((1, fit)), vm((1, fit), BF16),
        vm((owned, LANES), I32), vm((bands, 8, LANES)), vm((64, LANES), I32),
        vm((units * AXIS, LANES), I32),
        vm((fit, AXIS * LANES), BF16), vm((AXIS * LANES, LANES), BF16),
        vm((chunks, 2 * LANES, span), BF16), vm((chunks, 3 * pairs, span), BF16),
        vm((64, 32), BF16), vm((128, 64), BF16), vm((32, 128), BF16), vm((64, 256), BF16),
        vm((3, rows, row_lanes)), vm((tiles, rows, LANES)), vm((rows, row_lanes)),
        vm((tiles, rows, LANES), I32), vm((3, rows, row_lanes)),
        vm((tiles, 8 * rows, LANES)), vm((tiles, 8 * rows, LANES)),
        vm((chunks, 32, span)), vm((chunks, 64, span), BF16), vm((chunks, 128, span), BF16),
        vm((chunks, 128, span), BF16), vm((4 * owned, LANES)), vm((4 * AXIS, owned, LANES)),
        vm((owned, AXIS * LANES), BF16), vm((owned, AXIS * LANES)),
        vm((4 * owned, AXIS * LANES), BF16), vm((4 * owned, LANES)),
        vm((tiles, 8 * rows, LANES)), vm((tiles, rows, LANES)),
        vm((tiles, 16 * rows, LANES)), vm((tiles, 16 * rows, LANES)), vm((32 * bands, span), BF16),
        vm((bands, 16, LANES)), vm((slots, 16, LANES)), vm((16, LANES)), vm((models, 16, LANES)),
        pltpu.SemaphoreType.DMA((len(args),)),
    ]
    scratch += [pltpu.SemaphoreType.DMA((slots,))] * 6 + [pltpu.SemaphoreType.DMA((models,))] * 2
    return pl.pallas_call(
        functools.partial(
            kernel, count, models, strides, found, (owned, k_total, width, fit)
        ),
        out_shape=(
            jax.ShapeDtypeStruct((3, 1, 1, quarter), F32),
            jax.ShapeDtypeStruct((1, 1, quarter), F32),
            jax.ShapeDtypeStruct((1, 1, quarter), F32),
        ),
        in_specs=[ANY] * len(args),
        out_specs=(VM, VM, VM),
        scratch_shapes=scratch,
        compiler_params=pltpu.CompilerParams(
            collective_id=0, has_side_effects=True, vmem_limit_bytes=60000000
        ),
        name="forces",
    )(*args)


def solution(mesh):
    flat, deep = P("mp", None), P("mp", None, None)
    return jax.shard_map(
        local,
        mesh=mesh,
        in_specs=(
            P(None, "space"), P("space", None, None), P(None, "space"),
            flat, flat, deep, flat, deep, flat, deep, flat, deep, flat, deep, flat, flat,
        ),
        out_specs=(P(None, "space", "mp", None), P("space", "mp", None), P("space", "mp", None)),
        check_vma=False,
    )
```

```python
import functools
import math

import jax
import jax.numpy as jnp
from jax import lax
from jax.experimental import pallas as pl
from jax.experimental.pallas import tpu as pltpu
from jax.sharding import PartitionSpec as P

AXIS = 16
SOFTEN = 0.04
LANES = 128
ROWS = 2
ONE = 20.0
MESH = pl.DeviceIdType.MESH
F32 = jnp.float32
BF16 = jnp.bfloat16
I32 = jnp.int32
ANY = pl.BlockSpec(memory_space=pl.ANY)
VM = pl.BlockSpec(memory_space=pltpu.VMEM)


def dims(space_count):
    grid_y = min(4, max(2, space_count // 16))
    strides = (grid_y * grid_y, grid_y, 1)
    span = (-1, 0, 1)
    found = sorted(
        {
            (a * strides[0] + b * strides[1] + c * strides[2]) % space_count
            for a in span
            for b in span
            for c in span
        }
    )
    return strides, found


def nn(a, b):
    return jnp.dot(a, b, preferred_element_type=F32)


def nt(a, b):
    return lax.dot_general(a, b, (((1,), (1,)), ((), ())), preferred_element_type=F32)


def tn(a, b):
    return lax.dot_general(a, b, (((0,), (0,)), ((), ())), preferred_element_type=F32)


def iota(shape, dim):
    return lax.broadcasted_iota(I32, shape, dim)


def hot(mask):
    return jnp.where(mask, 1.0, 0.0).astype(BF16)


def spread_of(rows, units, width, group, flip=False):
    shape = (units, rows) if flip else (rows, units)
    row = iota(shape, 1 if flip else 0)
    unit = iota(shape, 0 if flip else 1)
    inner = row % group
    return (inner < width) & (unit == (row // group) * width + inner)


def column(mask, row_value):
    return jnp.sum(jnp.where(mask, row_value, 0.0), axis=1, keepdims=True)


def rounded(value):
    return value.astype(BF16).astype(F32)


def split(value, parts):
    pieces = []
    for _ in range(parts):
        piece = value.astype(BF16)
        pieces.append(piece)
        value = value - piece.astype(F32)
    return pieces


def both(value):
    return jnp.concatenate(split(value, 2), axis=0)


def lookup(row, lane):
    return jnp.take_along_axis(
        jnp.broadcast_to(row, lane.shape), lane, axis=1, mode="promise_in_bounds"
    )


def with_bias(weight, bias, width):
    col = iota(weight.shape, 1)
    for place, piece in enumerate(split(bias, 3)):
        weight = jnp.where(col == width + place, piece.astype(F32), weight)
    return weight.astype(BF16)


def kernel(
    count, models, strides, found, sizes,
    pos_in, list_in, nb_in,
    scale_in, shift_in, mid_in, midb_in, outer_in, outb_in,
    f1_in, f1b_in, f2_in, f2b_in, f3_in, f3b_in, read_in,
    out_ref,
    pos_all, list_all, nb_ref, scale_ref, shift_ref, mid_ref, midb_ref, outer_ref, outb_ref,
    f1_ref, f1b_ref, f2_ref, f2b_ref, f3_ref, f3b_ref, read_ref,
    nscr, ptab, code_ref, to_ref, f1p_ref, sel_ref, oh_ref, em_ref,
    w2_ref, w3_ref, a2_ref, a3_ref,
    off_ref, inv_ref, there_ref, id_ref, cen_ref, e4h_ref, e4l_ref,
    t1_ref, s2_ref, s3_ref, h3_ref, ms_ref, bm_ref, d_ref, dd_ref, y_ref, dms_ref,
    de4_ref, di_ref, th_ref, tl_ref, lhs_ref, mess_ref, held,
    local_sem, send_a, recv_a, send_b, recv_b, send_c, recv_c,
):
    owned, k_total, width, fit = sizes
    slots = len(found)
    group = LANES // math.gcd(k_total, LANES)
    tiles = group * k_total // LANES
    rows = owned // group
    chunks = rows // ROWS
    span = ROWS * tiles * LANES
    units = 4 * width
    g1, g2, g3 = 32, 64, 128
    pairs = ROWS * group * 4
    masks_count = (slots * owned + LANES - 1) // LANES
    me = lax.axis_index("space")
    model = lax.axis_index("mp")

    barrier = pltpu.get_barrier_semaphore()
    for off in found[1:]:
        pl.semaphore_signal(
            barrier, inc=1, device_id={"space": lax.rem(me + off, count)}, device_id_type=MESH
        )
    for step in range(1, models):
        pl.semaphore_signal(
            barrier, inc=1, device_id={"mp": lax.rem(model + step, models)}, device_id_type=MESH
        )
    moves = [
        (pos_in, pos_all.at[0]), (list_in, list_all.at[0]), (nb_in, nb_ref),
        (scale_in, scale_ref), (shift_in, shift_ref), (mid_in.at[0], mid_ref), (midb_in, midb_ref),
        (outer_in.at[0], outer_ref), (outb_in, outb_ref), (f1_in.at[0], f1_ref), (f1b_in, f1b_ref),
        (f2_in.at[0], f2_ref), (f2b_in, f2b_ref), (f3_in.at[0], f3_ref), (f3b_in, f3b_ref),
        (read_in, read_ref),
    ]
    fetched = []
    for place, (src, dst) in enumerate(moves):
        copy = pltpu.make_async_copy(src, dst, local_sem.at[place])
        copy.start()
        fetched.append(copy)
    for copy in fetched[:2]:
        copy.wait()
    pl.semaphore_wait(barrier, len(found) - 1 + models - 1)
    shares = []
    for slot, off in enumerate(found):
        if off == 0:
            continue
        peer = lax.rem(me + count - off, count)
        for ref, send, recv in ((pos_all, send_a, recv_a), (list_all, send_b, recv_b)):
            copy = pltpu.make_async_remote_copy(
                src_ref=ref.at[0],
                dst_ref=ref.at[slot],
                send_sem=send.at[slot],
                recv_sem=recv.at[slot],
                device_id={"space": peer},
                device_id_type=MESH,
            )
            copy.start()
            shares.append(copy)

    em_ref[...] = jnp.zeros_like(em_ref)
    th_ref[...] = jnp.zeros_like(th_ref)
    tl_ref[...] = jnp.zeros_like(tl_ref)
    nscr[...] = jnp.zeros_like(nscr)
    ptab[...] = jnp.zeros_like(ptab)
    for copy in fetched[2:9]:
        copy.wait()
    c1 = spread_of(g1, width, width, g1)
    r2 = spread_of(g2, 2 * width, width, g1)
    r3 = spread_of(g3, 4 * width, width, g1)
    scale_c, shift_c = column(c1, scale_ref[...]), column(c1, shift_ref[...])
    unit_row = iota((g1, 1), 0)
    shift_c = jnp.where((unit_row >= width) & (unit_row < width + 3), ONE, shift_c)
    bias2_c, bias3_c = column(r2, midb_ref[...]), column(r3, outb_ref[...])
    wide1 = hot(spread_of(g1, width, width, g1, True))
    wide2 = hot(spread_of(g2, 2 * width, width, g1, True))
    wide3 = hot(spread_of(g3, 4 * width, width, g1, True))
    mid_t, outer_t = mid_ref[...], outer_ref[...]
    w2 = nn(nt(hot(r2), mid_t).astype(BF16), wide1)
    w2t = nn(nn(hot(c1), mid_t).astype(BF16), wide2)
    w3 = nn(nt(hot(r3), outer_t).astype(BF16), wide2)
    w3t = nn(nn(hot(r2), outer_t).astype(BF16), wide3)
    w2_ref[...] = with_bias(w2, bias2_c, width)
    w3_ref[...] = with_bias(w3, bias3_c, width)
    fold2 = hot(iota((g1, g2), 1) % g1 == iota((g1, g2), 0))
    fold3 = hot(iota((g2, g3), 1) % g2 == iota((g2, g3), 0))
    a2_ref[...] = jnp.concatenate([w2t.astype(BF16), fold2], axis=1)
    a3_ref[...] = jnp.concatenate([w3t.astype(BF16), fold3], axis=1)

    nscr[:, 0:k_total] = nb_ref[...]
    lane = iota((rows, LANES), 1)
    own_row = iota((rows, LANES), 0)
    turned = [
        pltpu.roll(nscr[a * rows : (a + 1) * rows, :], (k_total * a) % LANES, 1) if (k_total * a) % LANES
        else nscr[a * rows : (a + 1) * rows, :]
        for a in range(group)
    ]
    member = []
    wanted = []
    for tile in range(tiles):
        place = lane + tile * LANES
        which = jnp.zeros_like(lane)
        for a in range(1, group):
            which = which + jnp.where(place >= a * k_total, 1, 0)
        member.append(which)
        value = turned[0]
        for a in range(1, group):
            value = jnp.where(which == a, turned[a], value)
        wanted.append(value)

    own_pos = jnp.concatenate([pos_all[0], jnp.zeros((3, LANES - owned), F32)], axis=1)
    for tile in range(tiles):
        at = member[tile] * rows + own_row
        for c in range(3):
            cen_ref[c, :, tile * LANES : (tile + 1) * LANES] = lookup(own_pos[c : c + 1], at)

    fetched[9].wait()

    source = iota((units * AXIS, LANES), 0)
    unit = source >> 4
    padded = unit
    for a in range(1, 4):
        padded = padded + jnp.where(unit >= a * width, g1 - width, 0)
    to_ref[...] = padded + LANES * (source & (AXIS - 1)) - iota((units * AXIS, LANES), 1)

    def order(step):
        target = to_ref[...]
        pick = jnp.concatenate(
            [hot(target == LANES * (2 * step)), hot(target == LANES * (2 * step + 1))], axis=1
        )
        f1p_ref[:, pl.ds(pl.multiple_of(step * 2 * LANES, 2 * LANES), 2 * LANES)] = nn(
            f1_ref[...], pick
        ).astype(BF16)

    for step in range(AXIS // 2):
        order(step)
    sel_ref[...] = hot((iota(sel_ref.shape, 0) >> 7) == iota(sel_ref.shape, 1))

    def own_hot(step):
        for inner in range(ROWS):
            r = step * ROWS + inner
            for tile in range(tiles):
                at = slice((inner * tiles + tile) * LANES, (inner * tiles + tile + 1) * LANES)
                which = member[tile][0:1] * rows + r
                oh_ref[step, LANES : 2 * LANES, at] = hot(iota((LANES, LANES), 0) == which)

    for step in range(chunks):
        own_hot(step)
    for copy in fetched[10:]:
        copy.wait()

    for copy in shares:
        copy.wait_recv()

    base = sum(1 << (16 + 2 * s) for s in range(3))
    where = {off: slot for slot, off in enumerate(found)}

    def neighbour(off, section, side):
        return (off + (-strides[section] if side == 0 else strides[section])) % count

    needs = (
        sorted({(b * strides[1] + c * strides[2]) % count for b in (-1, 0, 1) for c in (-1, 0, 1)}),
        sorted({(c * strides[2]) % count for c in (-1, 0, 1)}),
        [0],
    )
    place = {}
    for section in range(3):
        for off in needs[section]:
            for side in range(2):
                place[(off, 2 * section + side)] = len(place)
    for section in range(3):
        todo = [(off, side) for off in needs[section] for side in range(2)]
        if section == 0:
            for off, side in todo:
                source = neighbour(off, section, side)
                slot = where[source]
                shift = (-1 if side == 0 else 1) << (16 + 2 * section)
                at = place[(off, side)]
                code_ref[at : at + 1, :] = list_all[slot, side] + (slot * owned + base + shift)
            continue
        names, bases, tables = [], [], [[] for _ in range(2 * section)]
        for off, side in todo:
            source = neighbour(off, section, side)
            slot = where[source]
            names.append(list_all[slot, 2 * section + side])
            shift = (-1 if side == 0 else 1) << (16 + 2 * section)
            bases.append((slot * owned + base, shift))
            for block in range(2 * section):
                at = place[(source, block)]
                tables[block].append(code_ref[at : at + 1, :])
        for index, (off, side) in enumerate(todo):
            name = jnp.broadcast_to(names[index], (8, LANES))
            moved = jnp.where(name >= owned, name + (LANES - owned), name)
            row = moved >> 7
            spot = moved & (LANES - 1)
            result = name + bases[index][0]
            for block in range(2 * section):
                result = jnp.where(row == block + 1, lookup(tables[block][index], spot), result)
            at = place[(off, 2 * section + side)]
            code_ref[at : at + 1, :] = result[0:1] + bases[index][1]

    for slot in range(slots):
        at = (slot * owned) % LANES
        ptab[(slot * owned) // LANES, 0:3, at : at + owned] = pos_all[slot]

    for tile in range(tiles):
        cut = slice(tile * LANES, (tile + 1) * LANES)
        j = wanted[tile]
        there = jnp.where(j >= 0, 1.0, 0.0)
        moved = jnp.where(j >= owned, j + (LANES - owned), j)
        row = moved >> 7
        spot = moved & (LANES - 1)
        code = j + base
        for block in range(6):
            at = place[(0, block)]
            code = jnp.where(row == block + 1, lookup(code_ref[at : at + 1, :], spot), code)
        code = jnp.where(j >= 0, code, base)
        ident = code & 65535
        id_ref[tile] = ident
        prow = ident >> 7
        spot = ident & (LANES - 1)
        offs = []
        for c in range(3):
            value = lookup(ptab[0, c : c + 1, :], spot)
            for part in range(1, ptab.shape[0]):
                value = jnp.where(prow == part, lookup(ptab[part, c : c + 1, :], spot), value)
            moved_by = (((code >> (16 + 2 * c)) & 3) - 1).astype(F32)
            offs.append((value + moved_by) - cen_ref[c, :, cut])
        radius = offs[0] * offs[0] + offs[1] * offs[1] + offs[2] * offs[2] + SOFTEN
        inv = lax.rsqrt(radius)
        near = there * inv
        far = near * inv
        there_ref[:, cut] = there
        inv_ref[tile] = inv
        for c in range(4):
            env = near if c == 0 else far * offs[c - 1]
            high = rounded(env)
            low = env - high
            if c > 0:
                off_ref[c - 1, :, cut] = offs[c - 1]
            for twice in range(2):
                e4h_ref[tile, pl.ds(4 * twice + c, rows, stride=8), :] = high
                e4l_ref[tile, pl.ds(4 * twice + c, rows, stride=8), :] = low

    sub8 = iota((8, LANES), 0) >> 2
    picks = [
        [member[tile][0:8] == 2 * v + sub8 for v in range(group // 2)] for tile in range(tiles)
    ]
    w2, w3 = w2_ref[...], w3_ref[...]

    def forward(ch):
        inv = jnp.concatenate(
            [inv_ref[tile, pl.ds(ch * ROWS + inner, 1), :] for inner in range(ROWS) for tile in range(tiles)],
            axis=1,
        )
        t1 = jnp.tanh(scale_c * inv + shift_c)
        t1_ref[ch] = t1
        h1 = t1.astype(BF16)
        h1f = h1.astype(F32)
        u2 = jnp.tanh(nn(w2, h1))
        h2 = (jnp.concatenate([h1f, h1f], axis=0) + u2).astype(BF16)
        s2_ref[ch] = (1.0 - u2 * u2).astype(BF16)
        u3 = jnp.tanh(nn(w3, h2))
        h2f = h2.astype(F32)
        h3 = (jnp.concatenate([h2f, h2f], axis=0) + u3).astype(BF16)
        s3_ref[ch] = (1.0 - u3 * u3).astype(BF16)
        h3_ref[ch] = h3
        for inner in range(ROWS):
            r = ch * ROWS + inner
            for tile in range(tiles):
                cut = slice(tile * LANES, (tile + 1) * LANES)
                at = slice((inner * tiles + tile) * LANES, (inner * tiles + tile + 1) * LANES)
                for part, ref in enumerate((e4h_ref, e4l_ref)):
                    value = ref[tile, pl.ds(pl.multiple_of(r * 8, 8), 8), :]
                    block = jnp.concatenate(
                        [jnp.where(pick, value, 0.0) for pick in picks[tile]], axis=0
                    ).astype(BF16)
                    size = 4 * group
                    em_ref[ch, part * pairs + inner * size : part * pairs + (inner + 1) * size, at] = block
                    if part == 0:
                        em_ref[ch, 2 * pairs + inner * size : 2 * pairs + (inner + 1) * size, at] = block
                ident = id_ref[tile, pl.ds(r, 1), :] & (LANES - 1)
                oh_ref[ch, 0:LANES, at] = hot(iota((LANES, LANES), 0) == ident)
        moment = nt(em_ref[ch, 0 : 2 * pairs, :], h3)
        ms_ref[pl.ds(pl.multiple_of(ch * pairs, pairs), pairs), :] = (
            moment[0:pairs] + moment[pairs : 2 * pairs]
        )

    for ch in range(chunks):
        forward(ch)

    inverse_k = 1.0 / k_total
    mt = [ms_ref[pl.ds(c, owned, stride=4), :] * inverse_k for c in range(4)]
    for p in range(AXIS):
        total_p = None
        for c in range(4):
            wide = jnp.broadcast_to(mt[c][:, p : p + 1], (owned, LANES))
            bm_ref[c * AXIS + p] = wide
            part = mt[c] * wide
            total_p = part if total_p is None else total_p + part
        d_ref[:, p * LANES : (p + 1) * LANES] = total_p.astype(BF16)

    u1 = jnp.tanh(nt(d_ref[...], f1p_ref[...]) + f1b_ref[...])
    q1 = u1.astype(BF16)
    u2 = jnp.tanh(nt(q1, f2_ref[...]) + f2b_ref[...])
    q2 = (q1.astype(F32) + u2).astype(BF16)
    u3 = jnp.tanh(nt(q2, f3_ref[...]) + f3b_ref[...])
    read = read_ref[...].astype(F32)

    def back(value, weight):
        pair = nn(both(value), weight)
        return rounded(pair[0:owned] + pair[owned : 2 * owned])

    b2 = read + back(read * ((1.0 + u3) * (1.0 - u3)), f3_ref[...])
    b1 = rounded(b2) + back(b2 * ((1.0 + u2) * (1.0 - u2)), f2_ref[...])
    dd_ref[...] = back(b1 * ((1.0 + u1) * (1.0 - u1)), f1p_ref[...])

    sums = [None] * 4
    for p in range(AXIS):
        dd = dd_ref[:, p * LANES : (p + 1) * LANES]
        for c in range(4):
            part = dd * bm_ref[c * AXIS + p]
            sums[c] = part if sums[c] is None else sums[c] + part
            y_ref[c * owned : (c + 1) * owned, p * LANES : (p + 1) * LANES] = (dd * mt[c]).astype(BF16)
    piled = nn(y_ref[...], sel_ref[...])
    for c in range(4):
        dms_ref[pl.ds(c, owned, stride=4), :] = (sums[c] + piled[c * owned : (c + 1) * owned]) * inverse_k

    a2, a3 = a2_ref[...], a3_ref[...]

    def backward(ch):
        high, low = split(dms_ref[pl.ds(pl.multiple_of(ch * pairs, pairs), pairs), :], 2)
        h3 = h3_ref[ch]
        d3 = tn(jnp.concatenate([high, high, low], axis=0), em_ref[ch]).astype(BF16)
        p3 = d3 * s3_ref[ch]
        d2 = nn(a3, jnp.concatenate([p3, d3], axis=0)).astype(BF16)
        p2 = d2 * s2_ref[ch]
        d1 = nn(a2, jnp.concatenate([p2, d2], axis=0))
        t1 = t1_ref[ch]
        p1 = jnp.sum(d1 * (1.0 - t1 * t1) * scale_c, axis=0, keepdims=True)
        denv = nn(jnp.concatenate([high, low], axis=0), h3)
        denv = denv[0:pairs] + denv[pairs : 2 * pairs]
        for inner in range(ROWS):
            r = ch * ROWS + inner
            for tile in range(tiles):
                at = (inner * tiles + tile) * LANES
                di_ref[tile, pl.ds(r, 1), :] = p1[:, at : at + LANES]
                value = None
                for v, pick in enumerate(picks[tile]):
                    first = inner * 4 * group + 8 * v
                    part = jnp.where(pick, denv[first : first + 8, at : at + LANES], 0.0)
                    value = part if value is None else value + part
                value = value + pltpu.roll(value, 4, 0)
                de4_ref[tile, pl.ds(pl.multiple_of(r * 8, 8), 8), :] = value

    for ch in range(chunks):
        backward(ch)

    for tile in range(tiles):
        cut = slice(tile * LANES, (tile + 1) * LANES)
        offs = [off_ref[a, :, cut] for a in range(3)]
        inv, there = inv_ref[tile], there_ref[:, cut]
        denv = [de4_ref[tile, pl.ds(c, rows, stride=8), :] for c in range(4)]
        near = there * inv
        far = near * inv
        mixed = denv[1] * offs[0] + denv[2] * offs[1] + denv[3] * offs[2]
        dinv = di_ref[tile] + there * denv[0] + 2.0 * near * mixed
        pull = dinv * (inv * inv * inv)
        grads = [far * denv[a + 1] - pull * offs[a] for a in range(3)]
        terms = [-one for one in grads]
        terms += [-(offs[a] * grads[b]) for a in range(3) for b in range(3)]
        for at, term in enumerate(terms):
            high = rounded(term)
            th_ref[tile, pl.ds(at, rows, stride=16), :] = high
            tl_ref[tile, pl.ds(at, rows, stride=16), :] = term - high

    def scatter(ch, sums):
        for inner in range(ROWS):
            r = ch * ROWS + inner
            for tile in range(tiles):
                cut = slice(tile * LANES, (tile + 1) * LANES)
                at = slice((inner * tiles + tile) * LANES, (inner * tiles + tile + 1) * LANES)
                band = jnp.broadcast_to(id_ref[tile, pl.ds(r, 1), :] >> 7, (16, LANES))
                for part, ref in enumerate((th_ref, tl_ref)):
                    value = ref[tile, pl.ds(pl.multiple_of(r * 16, 16), 16), :]
                    for m in range(masks_count):
                        first = (2 * m + part) * 16
                        lhs_ref[first : first + 16, at] = jnp.where(band == m, value, 0.0).astype(BF16)
        return sums + nt(lhs_ref[...], oh_ref[ch])

    sums = jnp.zeros((32 * masks_count, 2 * LANES), F32)
    for ch in range(chunks):
        sums = scatter(ch, sums)
    quarter = owned // models
    blocks = LANES // quarter
    lane8 = iota((8, LANES), 1)
    sub = iota((8, LANES), 0)
    spot = lane8 % quarter
    block = lane8 // quarter

    def across(value):
        value = jnp.take_along_axis(
            value, ((block - sub) & (blocks - 1)) * quarter + spot, axis=1, mode="promise_in_bounds"
        )
        value = jnp.take_along_axis(value, (block - sub) & (blocks - 1), axis=0, mode="promise_in_bounds")
        return jnp.take_along_axis(
            value, ((block + sub) & (blocks - 1)) * quarter + spot, axis=1, mode="promise_in_bounds"
        )

    centre = jnp.zeros((8, LANES), F32)
    wholes = []
    for m in range(masks_count):
        whole = sums[32 * m : 32 * m + 16] + sums[32 * m + 16 : 32 * m + 32]
        centre = centre + whole[0:8, LANES : 2 * LANES]
        wholes.append([whole[0:8, 0:LANES], whole[8:16, 0:LANES]])
    wholes[0][0] = wholes[0][0] - jnp.where(sub < 3, centre, 0.0)
    for m in range(masks_count):
        for half in range(2):
            turned_block = across(wholes[m][half])
            for at in range(blocks):
                mess_ref[m * blocks + at, half : half + 1, :] = turned_block[at : at + 1, :]

    sent = []
    for slot, off in enumerate(found):
        for step in range(models):
            if off == 0 and step == 0:
                continue
            to = lax.rem(model + step, models)
            index = step * slots + slot
            copy = pltpu.make_async_remote_copy(
                src_ref=mess_ref.at[slot * models + to],
                dst_ref=held.at[index],
                send_sem=send_c.at[index],
                recv_sem=recv_c.at[index],
                device_id={"mp": to, "space": lax.rem(me + off, count)},
                device_id_type=MESH,
            )
            copy.start()
            sent.append(copy)
    for copy in sent:
        copy.wait_recv()
    stacked = []
    for step in range(models):
        value = mess_ref[model] if step == 0 else held[step * slots]
        for slot in range(1, slots):
            value = value + held[step * slots + slot]
        stacked.append(value)
    mean = sum(stacked[1:], stacked[0]) * (1.0 / models)
    square = jnp.zeros_like(mean)
    for one in stacked:
        square = square + (one - mean) * (one - mean)
    square = square * (1.0 / models)
    part_of = iota((1, LANES), 1) // quarter
    force = jnp.where(part_of < 3, square[0:1], 0.0)
    virial = jnp.where(part_of >= 3, square[0:1], 0.0) + jnp.where(part_of < 12 - blocks, square[1:2], 0.0)
    two = jnp.concatenate([force, virial], axis=0)
    reach = LANES // 2
    while reach >= quarter:
        two = two + pltpu.roll(two, reach, 1)
        reach //= 2
    out_ref[0:1, :] = mean[0:1]
    out_ref[1:3, :] = two
    for copy in shares + sent:
        copy.wait_send()


def settle(out_in, mean_ref, force_ref, virial_ref):
    quarter = mean_ref.shape[-1]
    for c in range(3):
        mean_ref[c, 0] = out_in[0:1, c * quarter : (c + 1) * quarter]
    force_ref[0] = out_in[1:2, 0:quarter]
    virial_ref[0] = out_in[2:3, 0:quarter]


def local(positions, send_lists, neighbours, *weights):
    count = lax.axis_size("space")
    models = lax.axis_size("mp")
    strides, found = dims(count)
    slots = len(found)
    owned = positions.shape[1]
    k_total = neighbours.shape[0]
    width = weights[0].shape[1]
    units = 4 * width
    quarter = owned // models
    blocks, cap = send_lists.shape[1:]
    lists = jnp.transpose(send_lists, (1, 0, 2))
    named = neighbours.T
    scale, shift, mid, midb, outer, outb, f1, f1b, f2, f2b, f3, f3b, read = weights
    mid = jnp.swapaxes(mid, 1, 2)
    outer = jnp.swapaxes(outer, 1, 2)
    fit = f1.shape[1]
    group = LANES // math.gcd(k_total, LANES)
    rows = owned // group
    row_lanes = group * k_total
    tiles = row_lanes // LANES
    pairs = ROWS * group * 4
    bands = (slots * owned + LANES - 1) // LANES
    span = ROWS * row_lanes
    chunks = rows // ROWS
    args = (positions, lists, named, scale, shift, mid, midb, outer, outb, f1, f1b, f2, f2b, f3, f3b, read)

    def vm(shape, dtype=F32):
        return pltpu.VMEM(shape, dtype)

    scratch = [
        vm((slots, 3, owned)), vm((slots, blocks, 1, cap), I32), vm((owned, k_total), I32),
        vm((1, width)), vm((1, width)), vm((width, 2 * width), BF16), vm((1, 2 * width)),
        vm((2 * width, 4 * width), BF16), vm((1, 4 * width)),
        vm((fit, units * AXIS), BF16), vm((1, fit)), vm((fit, fit), BF16), vm((1, fit)),
        vm((fit, fit), BF16), vm((1, fit)), vm((1, fit), BF16),
        vm((owned, LANES), I32), vm((bands, 8, LANES)), vm((64, LANES), I32),
        vm((units * AXIS, LANES), I32),
        vm((fit, AXIS * LANES), BF16), vm((AXIS * LANES, LANES), BF16),
        vm((chunks, 2 * LANES, span), BF16), vm((chunks, 3 * pairs, span), BF16),
        vm((64, 32), BF16), vm((128, 64), BF16), vm((32, 128), BF16), vm((64, 256), BF16),
        vm((3, rows, row_lanes)), vm((tiles, rows, LANES)), vm((rows, row_lanes)),
        vm((tiles, rows, LANES), I32), vm((3, rows, row_lanes)),
        vm((tiles, 8 * rows, LANES)), vm((tiles, 8 * rows, LANES)),
        vm((chunks, 32, span)), vm((chunks, 64, span), BF16), vm((chunks, 128, span), BF16),
        vm((chunks, 128, span), BF16), vm((4 * owned, LANES)), vm((4 * AXIS, owned, LANES)),
        vm((owned, AXIS * LANES), BF16), vm((owned, AXIS * LANES)),
        vm((4 * owned, AXIS * LANES), BF16), vm((4 * owned, LANES)),
        vm((tiles, 8 * rows, LANES)), vm((tiles, rows, LANES)),
        vm((tiles, 16 * rows, LANES)), vm((tiles, 16 * rows, LANES)), vm((32 * bands, span), BF16),
        vm((bands * (LANES // quarter), 2, LANES)), vm((slots * models, 2, LANES)),
        pltpu.SemaphoreType.DMA((len(args),)),
    ]
    scratch += [pltpu.SemaphoreType.DMA((slots,))] * 4
    scratch += [pltpu.SemaphoreType.DMA((slots * models,))] * 2
    packed = pl.pallas_call(
        functools.partial(
            kernel, count, models, strides, found, (owned, k_total, width, fit)
        ),
        out_shape=jax.ShapeDtypeStruct((3, LANES), F32),
        in_specs=[ANY] * len(args),
        out_specs=VM,
        scratch_shapes=scratch,
        compiler_params=pltpu.CompilerParams(
            collective_id=0, has_side_effects=True, vmem_limit_bytes=60000000
        ),
        name="forces",
    )(*args)
    return pl.pallas_call(
        settle,
        out_shape=(
            jax.ShapeDtypeStruct((3, 1, 1, quarter), F32),
            jax.ShapeDtypeStruct((1, 1, quarter), F32),
            jax.ShapeDtypeStruct((1, 1, quarter), F32),
        ),
        in_specs=[VM],
        out_specs=(VM, VM, VM),
        name="settle",
    )(packed)


def solution(mesh):
    flat, deep = P("mp", None), P("mp", None, None)
    return jax.shard_map(
        local,
        mesh=mesh,
        in_specs=(
            P(None, "space"), P("space", None, None), P(None, "space"),
            flat, flat, deep, flat, deep, flat, deep, flat, deep, flat, deep, flat, flat,
        ),
        out_specs=(P(None, "space", "mp", None), P("space", "mp", None), P("space", "mp", None)),
        check_vma=False,
    )
```

```python
import functools
import math

import jax
import jax.numpy as jnp
from jax import lax
from jax.experimental import pallas as pl
from jax.experimental.pallas import tpu as pltpu
from jax.sharding import PartitionSpec as P

AXIS = 16
SOFTEN = 0.04
LANES = 128
ROWS = 2
ONE = 20.0
MESH = pl.DeviceIdType.MESH
F32 = jnp.float32
BF16 = jnp.bfloat16
I32 = jnp.int32
ANY = pl.BlockSpec(memory_space=pl.ANY)
VM = pl.BlockSpec(memory_space=pltpu.VMEM)


def dims(space_count):
    grid_y = min(4, max(2, space_count // 16))
    strides = (grid_y * grid_y, grid_y, 1)
    span = (-1, 0, 1)
    found = sorted(
        {
            (a * strides[0] + b * strides[1] + c * strides[2]) % space_count
            for a in span
            for b in span
            for c in span
        }
    )
    return strides, found


def nn(a, b):
    return jnp.dot(a, b, preferred_element_type=F32)


def nt(a, b):
    return lax.dot_general(a, b, (((1,), (1,)), ((), ())), preferred_element_type=F32)


def tn(a, b):
    return lax.dot_general(a, b, (((0,), (0,)), ((), ())), preferred_element_type=F32)


def iota(shape, dim):
    return lax.broadcasted_iota(I32, shape, dim)


def hot(mask):
    return jnp.where(mask, 1.0, 0.0).astype(BF16)


def spread_of(rows, units, width, group, flip=False):
    shape = (units, rows) if flip else (rows, units)
    row = iota(shape, 1 if flip else 0)
    unit = iota(shape, 0 if flip else 1)
    inner = row % group
    return (inner < width) & (unit == (row // group) * width + inner)


def column(mask, row_value):
    return jnp.sum(jnp.where(mask, row_value, 0.0), axis=1, keepdims=True)


def rounded(value):
    return value.astype(BF16).astype(F32)


def split(value, parts):
    pieces = []
    for _ in range(parts):
        piece = value.astype(BF16)
        pieces.append(piece)
        value = value - piece.astype(F32)
    return pieces


def both(value):
    return jnp.concatenate(split(value, 2), axis=0)


def lookup(row, lane):
    return jnp.take_along_axis(
        jnp.broadcast_to(row, lane.shape), lane, axis=1, mode="promise_in_bounds"
    )


def with_bias(weight, bias, width):
    col = iota(weight.shape, 1)
    for place, piece in enumerate(split(bias, 3)):
        weight = jnp.where(col == width + place, piece.astype(F32), weight)
    return weight.astype(BF16)


def kernel(
    count, models, strides, found, sizes,
    pos_in, list_in, nb_in,
    scale_in, shift_in, mid_in, midb_in, outer_in, outb_in,
    f1_in, f1b_in, f2_in, f2b_in, f3_in, f3b_in, read_in,
    out_ref,
    pos_all, list_all, nb_ref, scale_ref, shift_ref, mid_ref, midb_ref, outer_ref, outb_ref,
    f1_ref, f1b_ref, f2_ref, f2b_ref, f3_ref, f3b_ref, read_ref,
    nscr, ptab, code_ref, to_ref, f1p_ref, sel_ref, oh_ref, em_ref,
    w2_ref, w3_ref, a2_ref, a3_ref,
    off_ref, inv_ref, there_ref, id_ref, cen_ref, e4h_ref, e4l_ref,
    t1_ref, s2_ref, s3_ref, h3_ref, h1_ref, h2_ref, b3_ref, b2_ref, ms_ref, bm_ref, d_ref, dd_ref, y_ref, dms_ref,
    de4_ref, di_ref, th_ref, tl_ref, lhs_ref, mess_ref, held,
    local_sem, send_a, recv_a, send_b, recv_b, send_c, recv_c,
):
    owned, k_total, width, fit = sizes
    slots = len(found)
    group = LANES // math.gcd(k_total, LANES)
    tiles = group * k_total // LANES
    rows = owned // group
    chunks = rows // ROWS
    span = ROWS * tiles * LANES
    units = 4 * width
    g1, g2, g3 = 32, 64, 128
    pairs = ROWS * group * 4
    masks_count = (slots * owned + LANES - 1) // LANES
    me = lax.axis_index("space")
    model = lax.axis_index("mp")

    barrier = pltpu.get_barrier_semaphore()
    for off in found[1:]:
        pl.semaphore_signal(
            barrier, inc=1, device_id={"space": lax.rem(me + off, count)}, device_id_type=MESH
        )
    for step in range(1, models):
        pl.semaphore_signal(
            barrier, inc=1, device_id={"mp": lax.rem(model + step, models)}, device_id_type=MESH
        )
    moves = [
        (pos_in, pos_all.at[0]), (list_in, list_all.at[0]), (nb_in, nb_ref),
        (scale_in, scale_ref), (shift_in, shift_ref), (mid_in.at[0], mid_ref), (midb_in, midb_ref),
        (outer_in.at[0], outer_ref), (outb_in, outb_ref), (f1_in.at[0], f1_ref), (f1b_in, f1b_ref),
        (f2_in.at[0], f2_ref), (f2b_in, f2b_ref), (f3_in.at[0], f3_ref), (f3b_in, f3b_ref),
        (read_in, read_ref),
    ]
    fetched = []
    for place, (src, dst) in enumerate(moves):
        copy = pltpu.make_async_copy(src, dst, local_sem.at[place])
        copy.start()
        fetched.append(copy)
    for copy in fetched[:2]:
        copy.wait()
    pl.semaphore_wait(barrier, len(found) - 1 + models - 1)
    shares = []
    for slot, off in enumerate(found):
        if off == 0:
            continue
        peer = lax.rem(me + count - off, count)
        for ref, send, recv in ((pos_all, send_a, recv_a), (list_all, send_b, recv_b)):
            copy = pltpu.make_async_remote_copy(
                src_ref=ref.at[0],
                dst_ref=ref.at[slot],
                send_sem=send.at[slot],
                recv_sem=recv.at[slot],
                device_id={"space": peer},
                device_id_type=MESH,
            )
            copy.start()
            shares.append(copy)

    em_ref[...] = jnp.zeros_like(em_ref)
    th_ref[...] = jnp.zeros_like(th_ref)
    tl_ref[...] = jnp.zeros_like(tl_ref)
    nscr[...] = jnp.zeros_like(nscr)
    ptab[...] = jnp.zeros_like(ptab)
    for copy in fetched[2:9]:
        copy.wait()
    c1 = spread_of(g1, width, width, g1)
    r2 = spread_of(g2, 2 * width, width, g1)
    r3 = spread_of(g3, 4 * width, width, g1)
    scale_c, shift_c = column(c1, scale_ref[...]), column(c1, shift_ref[...])
    unit_row = iota((g1, 1), 0)
    shift_c = jnp.where((unit_row >= width) & (unit_row < width + 3), ONE, shift_c)
    bias2_c, bias3_c = column(r2, midb_ref[...]), column(r3, outb_ref[...])
    wide1 = hot(spread_of(g1, width, width, g1, True))
    wide2 = hot(spread_of(g2, 2 * width, width, g1, True))
    wide3 = hot(spread_of(g3, 4 * width, width, g1, True))
    mid_t, outer_t = mid_ref[...], outer_ref[...]
    w2 = nn(nt(hot(r2), mid_t).astype(BF16), wide1)
    w2t = nn(nn(hot(c1), mid_t).astype(BF16), wide2)
    w3 = nn(nt(hot(r3), outer_t).astype(BF16), wide2)
    w3t = nn(nn(hot(r2), outer_t).astype(BF16), wide3)
    w2_ref[...] = with_bias(w2, bias2_c, width)
    w3_ref[...] = with_bias(w3, bias3_c, width)
    fold2 = hot(iota((g1, g1), 1) == iota((g1, g1), 0))
    fold3 = hot(iota((g2, g2), 1) == iota((g2, g2), 0))
    a2_ref[...] = jnp.concatenate([w2t.astype(BF16), fold2], axis=1)
    a3_ref[...] = jnp.concatenate([w3t.astype(BF16), fold3], axis=1)

    nscr[:, 0:k_total] = nb_ref[...]
    lane = iota((rows, LANES), 1)
    own_row = iota((rows, LANES), 0)
    turned = [
        pltpu.roll(nscr[a * rows : (a + 1) * rows, :], (k_total * a) % LANES, 1) if (k_total * a) % LANES
        else nscr[a * rows : (a + 1) * rows, :]
        for a in range(group)
    ]
    member = []
    wanted = []
    for tile in range(tiles):
        place = lane + tile * LANES
        which = jnp.zeros_like(lane)
        for a in range(1, group):
            which = which + jnp.where(place >= a * k_total, 1, 0)
        member.append(which)
        value = turned[0]
        for a in range(1, group):
            value = jnp.where(which == a, turned[a], value)
        wanted.append(value)

    own_pos = jnp.concatenate([pos_all[0], jnp.zeros((3, LANES - owned), F32)], axis=1)
    for tile in range(tiles):
        at = member[tile] * rows + own_row
        for c in range(3):
            cen_ref[c, :, tile * LANES : (tile + 1) * LANES] = lookup(own_pos[c : c + 1], at)

    fetched[9].wait()

    source = iota((units * AXIS, LANES), 0)
    unit = source >> 4
    padded = unit
    for a in range(1, 4):
        padded = padded + jnp.where(unit >= a * width, g1 - width, 0)
    to_ref[...] = padded + LANES * (source & (AXIS - 1)) - iota((units * AXIS, LANES), 1)

    def order(step):
        target = to_ref[...]
        pick = jnp.concatenate(
            [hot(target == LANES * (2 * step)), hot(target == LANES * (2 * step + 1))], axis=1
        )
        f1p_ref[:, pl.ds(pl.multiple_of(step * 2 * LANES, 2 * LANES), 2 * LANES)] = nn(
            f1_ref[...], pick
        ).astype(BF16)

    for step in range(AXIS // 2):
        order(step)
    sel_ref[...] = hot((iota(sel_ref.shape, 0) >> 7) == iota(sel_ref.shape, 1))

    for copy in fetched[10:]:
        copy.wait()

    for copy in shares:
        copy.wait_recv()

    base = sum(1 << (16 + 2 * s) for s in range(3))
    where = {off: slot for slot, off in enumerate(found)}

    def neighbour(off, section, side):
        return (off + (-strides[section] if side == 0 else strides[section])) % count

    needs = (
        sorted({(b * strides[1] + c * strides[2]) % count for b in (-1, 0, 1) for c in (-1, 0, 1)}),
        sorted({(c * strides[2]) % count for c in (-1, 0, 1)}),
        [0],
    )
    place = {}
    for section in range(3):
        for off in needs[section]:
            for side in range(2):
                place[(off, 2 * section + side)] = len(place)
    for section in range(3):
        todo = [(off, side) for off in needs[section] for side in range(2)]
        if section == 0:
            for off, side in todo:
                source = neighbour(off, section, side)
                slot = where[source]
                shift = (-1 if side == 0 else 1) << (16 + 2 * section)
                at = place[(off, side)]
                code_ref[at : at + 1, :] = list_all[slot, side] + (slot * owned + base + shift)
            continue
        names, bases, tables = [], [], [[] for _ in range(2 * section)]
        for off, side in todo:
            source = neighbour(off, section, side)
            slot = where[source]
            names.append(list_all[slot, 2 * section + side])
            shift = (-1 if side == 0 else 1) << (16 + 2 * section)
            bases.append((slot * owned + base, shift))
            for block in range(2 * section):
                at = place[(source, block)]
                tables[block].append(code_ref[at : at + 1, :])
        for index, (off, side) in enumerate(todo):
            name = jnp.broadcast_to(names[index], (8, LANES))
            moved = jnp.where(name >= owned, name + (LANES - owned), name)
            row = moved >> 7
            spot = moved & (LANES - 1)
            result = name + bases[index][0]
            for block in range(2 * section):
                result = jnp.where(row == block + 1, lookup(tables[block][index], spot), result)
            at = place[(off, 2 * section + side)]
            code_ref[at : at + 1, :] = result[0:1] + bases[index][1]

    for slot in range(slots):
        at = (slot * owned) % LANES
        ptab[(slot * owned) // LANES, 0:3, at : at + owned] = pos_all[slot]

    for tile in range(tiles):
        cut = slice(tile * LANES, (tile + 1) * LANES)
        j = wanted[tile]
        there = jnp.where(j >= 0, 1.0, 0.0)
        moved = jnp.where(j >= owned, j + (LANES - owned), j)
        row = moved >> 7
        spot = moved & (LANES - 1)
        code = j + base
        for block in range(6):
            at = place[(0, block)]
            code = jnp.where(row == block + 1, lookup(code_ref[at : at + 1, :], spot), code)
        code = jnp.where(j >= 0, code, base)
        ident = code & 65535
        id_ref[tile] = ident
        prow = ident >> 7
        spot = ident & (LANES - 1)
        offs = []
        for c in range(3):
            value = lookup(ptab[0, c : c + 1, :], spot)
            for part in range(1, ptab.shape[0]):
                value = jnp.where(prow == part, lookup(ptab[part, c : c + 1, :], spot), value)
            moved_by = (((code >> (16 + 2 * c)) & 3) - 1).astype(F32)
            offs.append((value + moved_by) - cen_ref[c, :, cut])
        radius = offs[0] * offs[0] + offs[1] * offs[1] + offs[2] * offs[2] + SOFTEN
        inv = lax.rsqrt(radius)
        near = there * inv
        far = near * inv
        there_ref[:, cut] = there
        inv_ref[tile] = inv
        for c in range(4):
            env = near if c == 0 else far * offs[c - 1]
            high = rounded(env)
            low = env - high
            if c > 0:
                off_ref[c - 1, :, cut] = offs[c - 1]
            for twice in range(2):
                e4h_ref[tile, pl.ds(4 * twice + c, rows, stride=8), :] = high
                e4l_ref[tile, pl.ds(4 * twice + c, rows, stride=8), :] = low

    sub8 = iota((8, LANES), 0) >> 2
    picks = [
        [member[tile][0:8] == 2 * v + sub8 for v in range(group // 2)] for tile in range(tiles)
    ]
    w2, w3 = w2_ref[...], w3_ref[...]

    def first_layer(ch):
        inv = jnp.concatenate(
            [
                inv_ref[tile, ch * ROWS + inner : ch * ROWS + inner + 1, :]
                for inner in range(ROWS)
                for tile in range(tiles)
            ],
            axis=1,
        )
        t1 = jnp.tanh(scale_c * inv + shift_c)
        t1_ref[ch] = t1
        h1_ref[ch] = t1.astype(BF16)

    def second_layer(ch):
        h1 = h1_ref[ch]
        h1f = h1.astype(F32)
        u2 = jnp.tanh(nn(w2, h1))
        h2_ref[ch] = (jnp.concatenate([h1f, h1f], axis=0) + u2).astype(BF16)
        s2_ref[ch] = (1.0 - u2 * u2).astype(BF16)

    def third_layer(ch):
        h2 = h2_ref[ch]
        u3 = jnp.tanh(nn(w3, h2))
        h2f = h2.astype(F32)
        h3_ref[ch] = (jnp.concatenate([h2f, h2f], axis=0) + u3).astype(BF16)
        s3_ref[ch] = (1.0 - u3 * u3).astype(BF16)

    def envelopes(ch):
        for inner in range(ROWS):
            r = ch * ROWS + inner
            for tile in range(tiles):
                cut = slice(tile * LANES, (tile + 1) * LANES)
                at = slice((inner * tiles + tile) * LANES, (inner * tiles + tile + 1) * LANES)
                for part, ref in enumerate((e4h_ref, e4l_ref)):
                    value = ref[tile, pl.ds(pl.multiple_of(r * 8, 8), 8), :]
                    block = jnp.concatenate(
                        [jnp.where(pick, value, 0.0) for pick in picks[tile]], axis=0
                    ).astype(BF16)
                    size = 4 * group
                    em_ref[ch, part * pairs + inner * size : part * pairs + (inner + 1) * size, at] = block
                    if part == 0:
                        em_ref[ch, 2 * pairs + inner * size : 2 * pairs + (inner + 1) * size, at] = block

    def moments(ch):
        moment = nt(em_ref[ch, 0 : 2 * pairs, :], h3_ref[ch])
        ms_ref[ch * pairs : (ch + 1) * pairs, :] = moment[0:pairs] + moment[pairs : 2 * pairs]

    for stage in (first_layer, second_layer, envelopes, third_layer, moments):
        for ch in range(chunks):
            stage(ch)

    inverse_k = 1.0 / k_total
    mt = [ms_ref[pl.ds(c, owned, stride=4), :] * inverse_k for c in range(4)]
    for p in range(AXIS):
        total_p = None
        for c in range(4):
            wide = jnp.broadcast_to(mt[c][:, p : p + 1], (owned, LANES))
            bm_ref[c * AXIS + p] = wide
            part = mt[c] * wide
            total_p = part if total_p is None else total_p + part
        d_ref[:, p * LANES : (p + 1) * LANES] = total_p.astype(BF16)

    def one_hots(step):
        for inner in range(ROWS):
            r = step * ROWS + inner
            for tile in range(tiles):
                at = slice((inner * tiles + tile) * LANES, (inner * tiles + tile + 1) * LANES)
                which = member[tile][0:1] * rows + r
                ident = id_ref[tile, pl.ds(r, 1), :] & (LANES - 1)
                oh_ref[step, 0:LANES, at] = hot(iota((LANES, LANES), 0) == ident)
                oh_ref[step, LANES : 2 * LANES, at] = hot(iota((LANES, LANES), 0) == which)

    u1 = jnp.tanh(nt(d_ref[...], f1p_ref[...]) + f1b_ref[...])
    for step in range(chunks * 0 // 8, chunks * 2 // 8):
        one_hots(step)
    q1 = u1.astype(BF16)
    u2 = jnp.tanh(nt(q1, f2_ref[...]) + f2b_ref[...])
    for step in range(chunks * 2 // 8, chunks * 4 // 8):
        one_hots(step)
    q2 = (q1.astype(F32) + u2).astype(BF16)
    u3 = jnp.tanh(nt(q2, f3_ref[...]) + f3b_ref[...])
    for step in range(chunks * 4 // 8, chunks * 5 // 8):
        one_hots(step)
    read = read_ref[...].astype(F32)

    def back(value, weight):
        pair = nn(both(value), weight)
        return rounded(pair[0:owned] + pair[owned : 2 * owned])

    b2 = read + back(read * ((1.0 + u3) * (1.0 - u3)), f3_ref[...])
    for step in range(chunks * 5 // 8, chunks * 6 // 8):
        one_hots(step)
    b1 = rounded(b2) + back(b2 * ((1.0 + u2) * (1.0 - u2)), f2_ref[...])
    for step in range(chunks * 6 // 8, chunks * 7 // 8):
        one_hots(step)
    dd_ref[...] = back(b1 * ((1.0 + u1) * (1.0 - u1)), f1p_ref[...])
    for step in range(chunks * 7 // 8, chunks * 8 // 8):
        one_hots(step)

    sums = [None] * 4
    for p in range(AXIS):
        dd = dd_ref[:, p * LANES : (p + 1) * LANES]
        for c in range(4):
            part = dd * bm_ref[c * AXIS + p]
            sums[c] = part if sums[c] is None else sums[c] + part
            y_ref[c * owned : (c + 1) * owned, p * LANES : (p + 1) * LANES] = (dd * mt[c]).astype(BF16)
    piled = nn(y_ref[...], sel_ref[...])
    for c in range(4):
        dms_ref[pl.ds(c, owned, stride=4), :] = (sums[c] + piled[c * owned : (c + 1) * owned]) * inverse_k

    a2, a3 = a2_ref[...], a3_ref[...]

    def back_outer(ch):
        high, low = split(dms_ref[ch * pairs : (ch + 1) * pairs, :], 2)
        d3 = tn(jnp.concatenate([high, high, low], axis=0), em_ref[ch]).astype(BF16)
        b3_ref[ch, 0:g3] = d3 * s3_ref[ch]
        b3_ref[ch, g3 : g3 + g2] = d3[0:g2] + d3[g2:g3]

    def back_env(ch):
        denv = nn(both(dms_ref[ch * pairs : (ch + 1) * pairs, :]), h3_ref[ch])
        denv = denv[0:pairs] + denv[pairs : 2 * pairs]
        for inner in range(ROWS):
            r = ch * ROWS + inner
            for tile in range(tiles):
                at = (inner * tiles + tile) * LANES
                value = None
                for v, pick in enumerate(picks[tile]):
                    first = inner * 4 * group + 8 * v
                    part = jnp.where(pick, denv[first : first + 8, at : at + LANES], 0.0)
                    value = part if value is None else value + part
                value = value + pltpu.roll(value, 4, 0)
                de4_ref[tile, r * 8 : (r + 1) * 8, :] = value

    def back_middle(ch):
        d2 = nn(a3, b3_ref[ch]).astype(BF16)
        b2_ref[ch, 0:g2] = d2 * s2_ref[ch]
        b2_ref[ch, g2 : g2 + g1] = d2[0:g1] + d2[g1:g2]

    def back_inner(ch):
        d1 = nn(a2, b2_ref[ch])
        t1 = t1_ref[ch]
        p1 = jnp.sum(d1 * (1.0 - t1 * t1) * scale_c, axis=0, keepdims=True)
        for inner in range(ROWS):
            for tile in range(tiles):
                at = (inner * tiles + tile) * LANES
                di_ref[tile, ch * ROWS + inner : ch * ROWS + inner + 1, :] = p1[:, at : at + LANES]

    for stage in (back_outer, back_middle, back_env, back_inner):
        for ch in range(chunks):
            stage(ch)

    for tile in range(tiles):
        cut = slice(tile * LANES, (tile + 1) * LANES)
        offs = [off_ref[a, :, cut] for a in range(3)]
        inv, there = inv_ref[tile], there_ref[:, cut]
        denv = [de4_ref[tile, pl.ds(c, rows, stride=8), :] for c in range(4)]
        near = there * inv
        far = near * inv
        mixed = denv[1] * offs[0] + denv[2] * offs[1] + denv[3] * offs[2]
        dinv = di_ref[tile] + there * denv[0] + 2.0 * near * mixed
        pull = dinv * (inv * inv * inv)
        grads = [far * denv[a + 1] - pull * offs[a] for a in range(3)]
        terms = [-one for one in grads]
        terms += [-(offs[a] * grads[b]) for a in range(3) for b in range(3)]
        for at, term in enumerate(terms):
            high = rounded(term)
            th_ref[tile, pl.ds(at, rows, stride=16), :] = high
            tl_ref[tile, pl.ds(at, rows, stride=16), :] = term - high

    def banded(ch):
        for inner in range(ROWS):
            r = ch * ROWS + inner
            for tile in range(tiles):
                cut = slice(tile * LANES, (tile + 1) * LANES)
                at = slice((inner * tiles + tile) * LANES, (inner * tiles + tile + 1) * LANES)
                band = jnp.broadcast_to(id_ref[tile, pl.ds(r, 1), :] >> 7, (16, LANES))
                for part, ref in enumerate((th_ref, tl_ref)):
                    value = ref[tile, pl.ds(pl.multiple_of(r * 16, 16), 16), :]
                    for m in range(masks_count):
                        first = (2 * m + part) * 16
                        lhs_ref[ch, first : first + 16, at] = jnp.where(band == m, value, 0.0).astype(BF16)

    sums = jnp.zeros((32 * masks_count, 2 * LANES), F32)
    for ch in range(chunks):
        banded(ch)
    for ch in range(chunks):
        sums = sums + nt(lhs_ref[ch], oh_ref[ch])
    quarter = owned // models
    blocks = LANES // quarter
    lane8 = iota((8, LANES), 1)
    sub = iota((8, LANES), 0)
    spot = lane8 % quarter
    block = lane8 // quarter

    def across(value):
        value = jnp.take_along_axis(
            value, ((block - sub) & (blocks - 1)) * quarter + spot, axis=1, mode="promise_in_bounds"
        )
        value = jnp.take_along_axis(value, (block - sub) & (blocks - 1), axis=0, mode="promise_in_bounds")
        return jnp.take_along_axis(
            value, ((block + sub) & (blocks - 1)) * quarter + spot, axis=1, mode="promise_in_bounds"
        )

    centre = jnp.zeros((8, LANES), F32)
    wholes = []
    for m in range(masks_count):
        whole = sums[32 * m : 32 * m + 16] + sums[32 * m + 16 : 32 * m + 32]
        centre = centre + whole[0:8, LANES : 2 * LANES]
        wholes.append([whole[0:8, 0:LANES], whole[8:16, 0:LANES]])
    wholes[0][0] = wholes[0][0] - jnp.where(sub < 3, centre, 0.0)
    for m in range(masks_count):
        for half in range(2):
            turned_block = across(wholes[m][half])
            for at in range(blocks):
                mess_ref[m * blocks + at, half : half + 1, :] = turned_block[at : at + 1, :]

    sent = []
    for slot, off in enumerate(found):
        for step in range(models):
            if off == 0 and step == 0:
                continue
            to = lax.rem(model + step, models)
            index = step * slots + slot
            copy = pltpu.make_async_remote_copy(
                src_ref=mess_ref.at[slot * models + to],
                dst_ref=held.at[index],
                send_sem=send_c.at[index],
                recv_sem=recv_c.at[index],
                device_id={"mp": to, "space": lax.rem(me + off, count)},
                device_id_type=MESH,
            )
            copy.start()
            sent.append(copy)
    for copy in sent:
        copy.wait_recv()
    stacked = []
    for step in range(models):
        value = mess_ref[model] if step == 0 else held[step * slots]
        for slot in range(1, slots):
            value = value + held[step * slots + slot]
        stacked.append(value)
    mean = sum(stacked[1:], stacked[0]) * (1.0 / models)
    square = jnp.zeros_like(mean)
    for one in stacked:
        square = square + (one - mean) * (one - mean)
    square = square * (1.0 / models)
    part_of = iota((1, LANES), 1) // quarter
    force = jnp.where(part_of < 3, square[0:1], 0.0)
    virial = jnp.where(part_of >= 3, square[0:1], 0.0) + jnp.where(part_of < 12 - blocks, square[1:2], 0.0)
    two = jnp.concatenate([force, virial], axis=0)
    reach = LANES // 2
    while reach >= quarter:
        two = two + pltpu.roll(two, reach, 1)
        reach //= 2
    out_ref[0:1, :] = mean[0:1]
    out_ref[1:3, :] = two
    for copy in shares + sent:
        copy.wait_send()


def settle(out_in, mean_ref, force_ref, virial_ref):
    quarter = mean_ref.shape[-1]
    for c in range(3):
        mean_ref[c, 0] = out_in[0:1, c * quarter : (c + 1) * quarter]
    force_ref[0] = out_in[1:2, 0:quarter]
    virial_ref[0] = out_in[2:3, 0:quarter]


def local(positions, send_lists, neighbours, *weights):
    count = lax.axis_size("space")
    models = lax.axis_size("mp")
    strides, found = dims(count)
    slots = len(found)
    owned = positions.shape[1]
    k_total = neighbours.shape[0]
    width = weights[0].shape[1]
    units = 4 * width
    quarter = owned // models
    blocks, cap = send_lists.shape[1:]
    lists = jnp.transpose(send_lists, (1, 0, 2))
    named = neighbours.T
    scale, shift, mid, midb, outer, outb, f1, f1b, f2, f2b, f3, f3b, read = weights
    mid = jnp.swapaxes(mid, 1, 2)
    outer = jnp.swapaxes(outer, 1, 2)
    fit = f1.shape[1]
    group = LANES // math.gcd(k_total, LANES)
    rows = owned // group
    row_lanes = group * k_total
    tiles = row_lanes // LANES
    pairs = ROWS * group * 4
    bands = (slots * owned + LANES - 1) // LANES
    span = ROWS * row_lanes
    chunks = rows // ROWS
    args = (positions, lists, named, scale, shift, mid, midb, outer, outb, f1, f1b, f2, f2b, f3, f3b, read)

    def vm(shape, dtype=F32):
        return pltpu.VMEM(shape, dtype)

    scratch = [
        vm((slots, 3, owned)), vm((slots, blocks, 1, cap), I32), vm((owned, k_total), I32),
        vm((1, width)), vm((1, width)), vm((width, 2 * width), BF16), vm((1, 2 * width)),
        vm((2 * width, 4 * width), BF16), vm((1, 4 * width)),
        vm((fit, units * AXIS), BF16), vm((1, fit)), vm((fit, fit), BF16), vm((1, fit)),
        vm((fit, fit), BF16), vm((1, fit)), vm((1, fit), BF16),
        vm((owned, LANES), I32), vm((bands, 8, LANES)), vm((64, LANES), I32),
        vm((units * AXIS, LANES), I32),
        vm((fit, AXIS * LANES), BF16), vm((AXIS * LANES, LANES), BF16),
        vm((chunks, 2 * LANES, span), BF16), vm((chunks, 3 * pairs, span), BF16),
        vm((64, 32), BF16), vm((128, 64), BF16), vm((32, 96), BF16), vm((64, 192), BF16),
        vm((3, rows, row_lanes)), vm((tiles, rows, LANES)), vm((rows, row_lanes)),
        vm((tiles, rows, LANES), I32), vm((3, rows, row_lanes)),
        vm((tiles, 8 * rows, LANES)), vm((tiles, 8 * rows, LANES)),
        vm((chunks, 32, span)), vm((chunks, 64, span), BF16), vm((chunks, 128, span), BF16),
        vm((chunks, 128, span), BF16), vm((chunks, 32, span), BF16), vm((chunks, 64, span), BF16),
        vm((chunks, 192, span), BF16), vm((chunks, 96, span), BF16), vm((4 * owned, LANES)), vm((4 * AXIS, owned, LANES)),
        vm((owned, AXIS * LANES), BF16), vm((owned, AXIS * LANES)),
        vm((4 * owned, AXIS * LANES), BF16), vm((4 * owned, LANES)),
        vm((tiles, 8 * rows, LANES)), vm((tiles, rows, LANES)),
        vm((tiles, 16 * rows, LANES)), vm((tiles, 16 * rows, LANES)), vm((chunks, 32 * bands, span), BF16),
        vm((bands * (LANES // quarter), 2, LANES)), vm((slots * models, 2, LANES)),
        pltpu.SemaphoreType.DMA((len(args),)),
    ]
    scratch += [pltpu.SemaphoreType.DMA((slots,))] * 4
    scratch += [pltpu.SemaphoreType.DMA((slots * models,))] * 2
    packed = pl.pallas_call(
        functools.partial(
            kernel, count, models, strides, found, (owned, k_total, width, fit)
        ),
        out_shape=jax.ShapeDtypeStruct((3, LANES), F32),
        in_specs=[ANY] * len(args),
        out_specs=VM,
        scratch_shapes=scratch,
        compiler_params=pltpu.CompilerParams(
            collective_id=0, has_side_effects=True, vmem_limit_bytes=60000000
        ),
        name="forces",
    )(*args)
    return pl.pallas_call(
        settle,
        out_shape=(
            jax.ShapeDtypeStruct((3, 1, 1, quarter), F32),
            jax.ShapeDtypeStruct((1, 1, quarter), F32),
            jax.ShapeDtypeStruct((1, 1, quarter), F32),
        ),
        in_specs=[VM],
        out_specs=(VM, VM, VM),
        name="settle",
    )(packed)


def solution(mesh):
    flat, deep = P("mp", None), P("mp", None, None)
    return jax.shard_map(
        local,
        mesh=mesh,
        in_specs=(
            P(None, "space"), P("space", None, None), P(None, "space"),
            flat, flat, deep, flat, deep, flat, deep, flat, deep, flat, deep, flat, flat,
        ),
        out_specs=(P(None, "space", "mp", None), P("space", "mp", None), P("space", "mp", None)),
        check_vma=False,
    )
```
